256 devices in a mesh: south: 2 (over z_2), east: 4 (over z_1, core), down: 8 (over z_0, x), ens: 4 (over y).
Axes of the slice: x: 4, y: 4, z: 8 (z_0: 2, z_1: 2, z_2: 2; z = z_0 * 4 + z_1 * 2 + z_2), core: 2. Of those that a mesh axis runs over, the one named last changes fastest.
Arguments:
- density: float32 [32, 128, 512, 128], P(('ens', 'south'), 'east', 'down'), parts along dimension 0, may hold values from 0.2 to 1.8
- flow_j: float32 [32, 128, 512, 128], P(('ens', 'south'), 'east', 'down'), parts along dimension 0, may hold values from -0.3 to 0.3
- flow_i: float32 [32, 128, 512, 128], P(('ens', 'south'), 'east', 'down'), parts along dimension 0, may hold values from -0.3 to 0.3
- flow_k: float32 [32, 128, 512, 128], P(('ens', 'south'), 'east', 'down'), parts along dimension 0, may hold values from -0.3 to 0.3
Outputs:
- density_end: float32 [32, 128, 512, 128], P(('ens', 'south'), 'east', 'down'), parts along dimension 0
The draws below stay inside these ranges and needn't reach their ends.
There are 4 independent parts, one for each index of `ens`. The reference program is written for one: setup_inputs(seed, part) draws one part's arguments, and reference() takes and returns one part's arrays. A program takes and returns all parts, laid end to end along the dimension named above; each array names one. Nothing has to cross between parts.
All inputs are finite; a program needn't handle non-finite values.
Results may differ from the reference program's by a relative error of at most 0.00002.
Values sent between devices are 32-bit elements; how exact they have to be, the bound alone decides.
A program may use at most 192 MiB of HBM per device.

```python
import jax
import jax.numpy as jnp
from jax import lax

GRID_J = 8
GRID_I = 128
GRID_K = 512
SPECIES = 128
STEPS = 3


def levels(own_key, extent, split, low, top_value):
    def one(axis_at, blocks):
        draws = jax.random.uniform(jax.random.fold_in(jax.random.fold_in(own_key, 6), axis_at), (blocks,), jnp.float32, low / len(split), top_value / len(split))
        return jnp.repeat(jnp.exp(draws), extent[axis_at] // blocks).reshape((-1,) + (1,) * (len(extent) - axis_at - 1))

    gain = one(*split[0])
    for cut in split[1:]:
        gain = gain * one(*cut)
    return gain


def setup_inputs(seed: int = 0, part: int = 0) -> dict:
    keys = jax.random.split(jax.random.key(seed), 5)
    part_keys = jax.random.split(jax.random.fold_in(keys[4], part), 5)
    density = jnp.clip(0.2 + 1.5999999 * jax.random.uniform(part_keys[0], (GRID_J, GRID_I, GRID_K, SPECIES), jnp.float32) ** levels(part_keys[0], (GRID_J, GRID_I, GRID_K, SPECIES), ((0, 2), (1, 4), (2, 8)), -0.2, 0.2), 0.2, 1.8)
    flow_j = jnp.clip(jax.random.uniform(part_keys[1], (GRID_J, GRID_I, GRID_K, SPECIES), jnp.float32, -0.3, 0.3) * levels(part_keys[1], (GRID_J, GRID_I, GRID_K, SPECIES), ((0, 2), (1, 4), (2, 8)), -0.4, 0.0), -0.3, 0.3)
    flow_i = jnp.clip(jax.random.uniform(part_keys[2], (GRID_J, GRID_I, GRID_K, SPECIES), jnp.float32, -0.3, 0.3) * levels(part_keys[2], (GRID_J, GRID_I, GRID_K, SPECIES), ((0, 2), (1, 4), (2, 8)), -0.4, 0.0), -0.3, 0.3)
    flow_k = jnp.clip(jax.random.uniform(part_keys[3], (GRID_J, GRID_I, GRID_K, SPECIES), jnp.float32, -0.3, 0.3) * levels(part_keys[3], (GRID_J, GRID_I, GRID_K, SPECIES), ((0, 2), (1, 4), (2, 8)), -0.4, 0.0), -0.3, 0.3)
    return dict(density=density, flow_j=flow_j, flow_i=flow_i, flow_k=flow_k)


def inner_cells(values, dims):
    for dim in dims:
        values = lax.slice_in_dim(values, 1, values.shape[dim] - 1, axis=dim)
    return values


def side_cells(values, dim, start, dims):
    others = [other for other in dims if other != dim]
    values = inner_cells(values, others)
    return lax.slice_in_dim(values, start, start + values.shape[dim] - 2, axis=dim)


def advance(padded, flow_j, flow_i, flow_k):
    middle = inner_cells(padded, (0, 1, 2))
    lower = [side_cells(padded, dim, 0, (0, 1, 2)) for dim in (0, 1, 2)]
    upper = [side_cells(padded, dim, 2, (0, 1, 2)) for dim in (0, 1, 2)]
    slopes = [above - below for above, below in zip(upper, lower)]
    smooth_rate = 0.05
    spread = lower[0] + upper[0] + lower[1] + upper[1] + lower[2] + upper[2] - 6.0 * middle
    return middle - flow_j * slopes[0] - flow_i * slopes[1] - flow_k * slopes[2] + smooth_rate * spread


def reference(density, flow_j, flow_i, flow_k):
    for step in range(STEPS):
        density = advance(jnp.pad(density, ((1, 1), (1, 1), (1, 1), (0, 0)), mode="constant"), flow_j, flow_i, flow_k)
    return density
```

```python
import functools

import jax
import jax.numpy as jnp
from jax import lax
from jax.experimental import pallas as pl
from jax.experimental.pallas import tpu as pltpu
from jax.sharding import PartitionSpec as P

STEPS = 3
SMOOTH = 0.05
PAD = 8


def kernel(
    sizes, width, den, fj, fi, fk, out, field, flow, k_send, k_recv,
    load_sem, store_sem, south_send, south_recv, east_send, east_recv, down_send, down_recv,
):
    n_south, n_east, n_down = sizes
    nj, ni, nk, _ = den.shape
    chunks = ni // (2 * width)
    south, east, down = (lax.axis_index(a) for a in ("south", "east", "down"))
    has_west, has_east = east > 0, east < n_east - 1
    has_up, has_down = down > 0, down < n_down - 1
    inner_k = pl.ds(PAD, nk)

    def to(axis, index):
        return dict(device_id={axis: index}, device_id_type=pl.DeviceIdType.MESH)

    loads = [pltpu.make_async_copy(den, field.at[0, pl.ds(1, nj), pl.ds(1, ni), inner_k], load_sem.at[0])]
    for x, src in enumerate((fj, fi, fk)):
        loads.append(pltpu.make_async_copy(src, flow.at[x], load_sem.at[x + 1]))
    for copy in loads:
        copy.start()

    barrier = pltpu.get_barrier_semaphore()
    pl.semaphore_signal(barrier, inc=1, **to("south", 1 - south))

    @pl.when(has_west)
    def _():
        pl.semaphore_signal(barrier, inc=1, **to("east", east - 1))

    @pl.when(has_east)
    def _():
        pl.semaphore_signal(barrier, inc=1, **to("east", east + 1))

    @pl.when(has_up)
    def _():
        pl.semaphore_signal(barrier, inc=1, **to("down", down - 1))

    @pl.when(has_down)
    def _():
        pl.semaphore_signal(barrier, inc=1, **to("down", down + 1))

    outside_j = jnp.where(south == 0, 0, nj + 1)

    def clear(n, _):
        for t in range(STEPS):
            field[t, outside_j, n + 1, inner_k] = jnp.zeros((nk, 128), jnp.float32)
        return 0

    lax.fori_loop(0, ni, clear, 0)
    for edge, at in ((jnp.logical_not(has_west), 0), (jnp.logical_not(has_east), ni + 1)):
        @pl.when(edge)
        def _(at=at):
            for t in range(STEPS):
                for j in range(nj):
                    field[t, j + 1, at, inner_k] = jnp.zeros((nk, 128), jnp.float32)
    for edge, side in ((jnp.logical_not(has_up), 0), (jnp.logical_not(has_down), 1)):
        @pl.when(edge)
        def _(side=side):
            for t in range(STEPS):
                for c in range(chunks):
                    k_recv[t, side, c] = jnp.zeros(k_recv.shape[3:], jnp.float32)

    near = (has_west, has_east, has_up, has_down)
    pl.semaphore_wait(barrier, 1 + sum(jnp.where(h, 1, 0) for h in near))

    def row_of(c, seg):
        return c * width if seg == 0 else ni - width - c * width

    my_j = jnp.where(south == 0, nj - 1, 0)
    their_j = jnp.where(south == 0, 0, nj + 1)

    def south_copy(t, c, seg):
        r = row_of(c, seg)
        if isinstance(t, int) and t == 0:
            src = den.at[my_j, pl.ds(r, width)]
        else:
            src = field.at[t, my_j + 1, pl.ds(r + 1, width), inner_k]
        return pltpu.make_async_remote_copy(
            src_ref=src, dst_ref=field.at[t, their_j, pl.ds(r + 1, width), inner_k],
            send_sem=south_send.at[t, c, seg], recv_sem=south_recv.at[t, c, seg], **to("south", 1 - south))

    def east_copy(t, side):
        r, dst, other = (0, ni + 1, east - 1) if side == 0 else (ni - 1, 0, east + 1)
        if t == 0:
            src = den.at[:, r]
        else:
            src = field.at[t, pl.ds(1, nj), r + 1, inner_k]
        return pltpu.make_async_remote_copy(
            src_ref=src, dst_ref=field.at[t, pl.ds(1, nj), dst, inner_k],
            send_sem=east_send.at[t, side], recv_sem=east_recv.at[t, 1 - side], **to("east", other))

    def down_copy(t, c, side):
        other = down - 1 if side == 0 else down + 1
        return pltpu.make_async_remote_copy(
            src_ref=k_send.at[t, side, c], dst_ref=k_recv.at[t, 1 - side, c],
            send_sem=down_send.at[t, c, side], recv_sem=down_recv.at[t, c, 1 - side], **to("down", other))

    def each(cond_low, cond_high, fn):
        for side, cond in ((0, cond_low), (1, cond_high)):
            @pl.when(cond)
            def _(side=side):
                fn(side)

    def first(c, _):
        for seg in (0, 1):
            south_copy(0, c, seg).start()
        return 0

    lax.fori_loop(0, chunks, first, 0)
    each(has_west, has_east, lambda side: east_copy(0, side).start())

    def pack(t, c, seg, w):
        r = row_of(c, seg) + w
        for j in range(nj):
            at = (seg * width + w) * nj + j
            k_send[t, 0, c, pl.ds(at, 1)] = field[t, j + 1, r + 1, pl.ds(PAD, 1)]
            k_send[t, 1, c, pl.ds(at, 1)] = field[t, j + 1, r + 1, pl.ds(PAD + nk - 1, 1)]

    def unpack(t, c, seg, w):
        r = row_of(c, seg) + w
        for j in range(nj):
            at = (seg * width + w) * nj + j
            field[t, j + 1, r + 1, pl.ds(PAD - 1, 1)] = k_recv[t, 0, c, pl.ds(at, 1)]
            field[t, j + 1, r + 1, pl.ds(PAD + nk, 1)] = k_recv[t, 1, c, pl.ds(at, 1)]

    loads[0].wait()

    def first_pack(c, _):
        for seg in (0, 1):
            for w in range(width):
                pack(0, c, seg, w)
        return 0

    lax.fori_loop(0, chunks, first_pack, 0)
    for copy in loads[1:]:
        copy.wait()

    def first_down(c, _):
        each(has_up, has_down, lambda side: down_copy(0, c, side).start())
        return 0

    lax.fori_loop(0, chunks, first_down, 0)

    def advance(t, r):
        for b in range(nk // 8):
            at = pl.ds(PAD + 8 * b, 8)
            column = [field[t, j, r + 1, at] for j in range(nj + 2)]
            for j in range(nj):
                mid, j_low, j_high = column[j + 1], column[j], column[j + 2]
                i_low, i_high = field[t, j + 1, r, at], field[t, j + 1, r + 2, at]
                k_low = field[t, j + 1, r + 1, pl.ds(PAD + 8 * b - 1, 8)]
                k_high = field[t, j + 1, r + 1, pl.ds(PAD + 8 * b + 1, 8)]
                here = pl.ds(8 * b, 8)
                spread = j_low + j_high + i_low + i_high + k_low + k_high - 6.0 * mid
                value = (
                    mid - flow[0, j, r, here] * (j_high - j_low) - flow[1, j, r, here] * (i_high - i_low)
                    - flow[2, j, r, here] * (k_high - k_low) + SMOOTH * spread
                )
                field[t + 1, j + 1, r + 1, at] = value

    def store_copy(c, seg):
        r = row_of(c, seg)
        return pltpu.make_async_copy(
            field.at[STEPS, pl.ds(1, nj), pl.ds(r + 1, width), inner_k], out.at[:, pl.ds(r, width)],
            store_sem.at[c, seg])

    def send(t, c):
        for seg in (0, 1):
            south_copy(t, c, seg).start()
        each(has_up, has_down, lambda side: down_copy(t, c, side).start())

    def store(c):
        for seg in (0, 1):
            store_copy(c, seg).start()

    for t in range(STEPS):
        def chunk(c, _, t=t):
            for seg in (0, 1):
                south_copy(t, c, seg).wait_recv()
            each(has_up, has_down, lambda side: down_copy(t, c, 1 - side).wait_recv())

            @pl.when(c == 0)
            def _():
                each(has_west, has_east, lambda side: east_copy(t, 1 - side).wait_recv())

            for seg in (0, 1):
                for w in range(width):
                    unpack(t, c, seg, w)

            def rows(w, _):
                for seg in (0, 1):
                    advance(t, row_of(c, seg) + w)
                return 0

            lax.fori_loop(0, width, rows, 0)
            if t < STEPS - 1:
                for seg in (0, 1):
                    for w in range(width):
                        pack(t + 1, c, seg, w)

                @pl.when(c > 0)
                def _():
                    send(t + 1, c - 1)

                @pl.when(c == 1)
                def _():
                    each(has_west, has_east, lambda side: east_copy(t + 1, side).start())

                if t > 0:
                    @pl.when(c == 0)
                    def _():
                        send(t, chunks - 1)
            else:
                @pl.when(c == 0)
                def _():
                    send(t, chunks - 1)

                @pl.when(c > 0)
                def _():
                    store(c - 1)
            return 0

        lax.fori_loop(0, chunks, chunk, 0)
    store(chunks - 1)

    def finish(c, _):
        for seg in (0, 1):
            for t in range(STEPS):
                south_copy(t, c, seg).wait_send()
            store_copy(c, seg).wait()
        for t in range(STEPS):
            each(has_up, has_down, lambda side: down_copy(t, c, side).wait_send())
        return 0

    lax.fori_loop(0, chunks, finish, 0)
    for t in range(STEPS):
        each(has_west, has_east, lambda side: east_copy(t, side).wait_send())


def solution(mesh, width=2):
    sizes = tuple(mesh.shape[a] for a in ("south", "east", "down"))

    def per_device(density, flow_j, flow_i, flow_k):
        nj, ni, nk, ns = density.shape
        chunks = ni // (2 * width)
        dma = pltpu.SemaphoreType.DMA
        return pl.pallas_call(
            functools.partial(kernel, sizes, width),
            out_shape=jax.ShapeDtypeStruct(density.shape, density.dtype),
            in_specs=[pl.BlockSpec(memory_space=pl.ANY)] * 4,
            out_specs=pl.BlockSpec(memory_space=pl.ANY),
            scratch_shapes=[
                pltpu.VMEM((STEPS + 1, nj + 2, ni + 2, nk + 2 * PAD, ns), jnp.float32),
                pltpu.VMEM((3, nj, ni, nk, ns), jnp.float32),
                pltpu.VMEM((STEPS, 2, chunks, 2 * width * nj, ns), jnp.float32),
                pltpu.VMEM((STEPS, 2, chunks, 2 * width * nj, ns), jnp.float32),
                dma((4,)),
                dma((chunks, 2)),
                dma((STEPS, chunks, 2)),
                dma((STEPS, chunks, 2)),
                dma((STEPS, 2)),
                dma((STEPS, 2)),
                dma((STEPS, chunks, 2)),
                dma((STEPS, chunks, 2)),
            ],
            compiler_params=pltpu.CompilerParams(
                collective_id=0, has_side_effects=True, vmem_limit_bytes=60 * 1024 * 1024
            ),
            name="advect",
        )(density, flow_j, flow_i, flow_k)

    spec = P(("ens", "south"), "east", "down", None)
    return jax.shard_map(per_device, mesh=mesh, in_specs=(spec,) * 4, out_specs=spec, check_vma=False)
```

```python
import functools

import jax
import jax.numpy as jnp
from jax import lax
from jax.experimental import pallas as pl
from jax.experimental.pallas import tpu as pltpu
from jax.sharding import PartitionSpec as P

STEPS = 3
SMOOTH = 0.05
PAD = 8


def kernel(
    sizes, width, lead, den, fj, fi, fk, out, field, flow, k_send, k_recv, k_relay,
    load_sem, south_send, south_recv, east_send, east_recv, down_send, down_recv, relay_send, relay_recv,
):
    _, n_east, n_down = sizes
    nj, ni, nk, ns = den.shape
    chunks = ni // width
    half = n_down // 2
    relays = chunks % half == 0
    rounds = chunks // half
    south, east, down = (lax.axis_index(a) for a in ("south", "east", "down"))
    has_west, has_east = east > 0, east < n_east - 1
    has_up, has_down = down > 0, down < n_down - 1
    inner_k = pl.ds(PAD, nk)
    my_j = jnp.where(south == 0, nj - 1, 0)
    their_j = jnp.where(south == 0, 0, nj + 1)
    rest_j = jnp.where(south == 0, 0, 1)

    def to(axis, index):
        return dict(device_id={axis: index}, device_id_type=pl.DeviceIdType.MESH)

    def each(cond_low, cond_high, fn):
        for side, cond in ((0, cond_low), (1, cond_high)):
            @pl.when(cond)
            def _(side=side):
                fn(side)

    def row_of(c):
        return width * jnp.where(c == 0, 0, jnp.where(c == 1, chunks - 1, c - 1))

    lower = down < half
    at_seam = jnp.logical_or(down == half - 1, down == half)
    mine = lax.rem(down, half)
    own_end = jnp.where(lower, half - 1, half)
    far_end = jnp.where(lower, half, half - 1)
    far_base = jnp.where(lower, half, 0)
    own_base = jnp.where(lower, 0, half)
    own_side = jnp.where(lower, 0, 1)
    is_relay = jnp.logical_not(at_seam)

    barrier = pltpu.get_barrier_semaphore()

    def hello(cond, axis, index):
        @pl.when(cond)
        def _():
            pl.semaphore_signal(barrier, inc=1, **to(axis, index))

    pl.semaphore_signal(barrier, inc=1, **to("south", 1 - south))
    hello(has_west, "east", east - 1)
    hello(has_east, "east", east + 1)
    hello(has_up, "down", down - 1)
    hello(has_down, "down", down + 1)
    targets = 1 + sum(jnp.where(h, 1, 0) for h in (has_west, has_east, has_up, has_down))
    if relays:
        hello(is_relay, "down", own_end)
        for m in range(half):
            hello(jnp.logical_and(at_seam, far_end - far_base != m), "down", far_base + m)
        targets = targets + jnp.where(at_seam, half - 1, 1)

    loads = [
        pltpu.make_async_copy(den.at[my_j], field.at[0, my_j + 1, pl.ds(1, ni), inner_k], load_sem.at[0]),
        pltpu.make_async_copy(
            den.at[pl.ds(rest_j, nj - 1)], field.at[0, pl.ds(rest_j + 1, nj - 1), pl.ds(1, ni), inner_k], load_sem.at[1]),
    ]
    for x, src in enumerate((fj, fi, fk)):
        loads.append(pltpu.make_async_copy(src, flow.at[x], load_sem.at[x + 2]))
    for copy in loads:
        copy.start()

    outside_j = jnp.where(south == 0, 0, nj + 1)

    def clear(n, _):
        for t in range(STEPS):
            field[t, outside_j, n + 1, inner_k] = jnp.zeros((nk, ns), jnp.float32)
        return 0

    lax.fori_loop(0, ni, clear, 0)
    for edge, at in ((jnp.logical_not(has_west), 0), (jnp.logical_not(has_east), ni + 1)):
        @pl.when(edge)
        def _(at=at):
            for t in range(STEPS):
                for j in range(nj):
                    field[t, j + 1, at, inner_k] = jnp.zeros((nk, ns), jnp.float32)
    for edge, side in ((jnp.logical_not(has_up), 0), (jnp.logical_not(has_down), 1)):
        @pl.when(edge)
        def _(side=side):
            for t in range(STEPS):
                for c in range(chunks):
                    k_recv[t, side, c] = jnp.zeros(k_recv.shape[3:], jnp.float32)

    def south_copy(t, c):
        rows = pl.ds(row_of(c) + 1, width)
        return pltpu.make_async_remote_copy(
            src_ref=field.at[t, my_j + 1, rows, inner_k], dst_ref=field.at[t, their_j, rows, inner_k],
            send_sem=south_send.at[t, c], recv_sem=south_recv.at[t, c], **to("south", 1 - south))

    def east_copy(t, side):
        r, dst, other = (1, ni + 1, east - 1) if side == 0 else (ni, 0, east + 1)
        return pltpu.make_async_remote_copy(
            src_ref=field.at[t, pl.ds(1, nj), r, inner_k], dst_ref=field.at[t, pl.ds(1, nj), dst, inner_k],
            send_sem=east_send.at[t, side], recv_sem=east_recv.at[t, 1 - side], **to("east", other))

    def down_copy(t, c, side):
        other = down - 1 if side == 0 else down + 1
        return pltpu.make_async_remote_copy(
            src_ref=k_send.at[t, side, c], dst_ref=k_recv.at[t, 1 - side, c],
            send_sem=down_send.at[t, c, side], recv_sem=down_recv.at[t, c, 1 - side], **to("down", other))

    def detour_copy(t, c, side):
        return pltpu.make_async_remote_copy(
            src_ref=k_send.at[t, side, c], dst_ref=k_relay.at[t, c // half],
            send_sem=down_send.at[t, c, side], recv_sem=relay_recv.at[t, c // half],
            **to("down", own_base + lax.rem(c, half)))

    def hand_on_copy(t, q, side):
        return pltpu.make_async_remote_copy(
            src_ref=k_relay.at[t, q], dst_ref=k_recv.at[t, side, mine + q * half],
            send_sem=relay_send.at[t, q], recv_sem=down_recv.at[t, mine + q * half, side], **to("down", far_end))

    def send_down(t, c):
        def one(side):
            if not relays:
                down_copy(t, c, side).start()
                return
            crosses = down == (half if side == 0 else half - 1)
            around = jnp.logical_and(crosses, own_base + lax.rem(c, half) != own_end)

            @pl.when(around)
            def _():
                detour_copy(t, c, side).start()

            @pl.when(jnp.logical_not(around))
            def _():
                down_copy(t, c, side).start()

        each(has_up, has_down, one)

    def hand_on(t, n):
        if not relays:
            return

        @pl.when(jnp.logical_and(is_relay, lax.rem(n, half) == mine))
        def _():
            q = n // half
            pltpu.make_async_remote_copy(
                src_ref=k_relay.at[t, q], dst_ref=k_relay.at[t, q],
                send_sem=relay_send.at[t, q], recv_sem=relay_recv.at[t, q], **to("down", far_end)).wait_recv()
            hand_on_copy(t, q, own_side).start()

    def ends(t, c, w):
        r = row_of(c) + w + 1
        for j in range(nj):
            yield j + 1, r, pl.ds(w * nj + j, 1)

    def pack(t, c):
        def row(w, _):
            for j, r, at in ends(t, c, w):
                k_send[t, 0, c, at] = field[t, j, r, pl.ds(PAD, 1)]
                k_send[t, 1, c, at] = field[t, j, r, pl.ds(PAD + nk - 1, 1)]
            return 0

        lax.fori_loop(0, width, row, 0)

    def unpack(t, c):
        def row(w, _):
            for j, r, at in ends(t, c, w):
                field[t, j, r, pl.ds(PAD - 1, 1)] = k_recv[t, 0, c, at]
                field[t, j, r, pl.ds(PAD + nk, 1)] = k_recv[t, 1, c, at]
            return 0

        lax.fori_loop(0, width, row, 0)

    def advance(t, c, first, count):
        def row(w, _):
            r = row_of(c) + w
            for b in range(nk // 8):
                at, here = pl.ds(PAD + 8 * b, 8), pl.ds(8 * b, 8)
                column = [field[t, first + p, r + 1, at] for p in range(count + 2)]
                for p in range(count):
                    j = first + p
                    mid, j_low, j_high = column[p + 1], column[p], column[p + 2]
                    i_low, i_high = field[t, j + 1, r, at], field[t, j + 1, r + 2, at]
                    k_low = field[t, j + 1, r + 1, pl.ds(PAD + 8 * b - 1, 8)]
                    k_high = field[t, j + 1, r + 1, pl.ds(PAD + 8 * b + 1, 8)]
                    spread = j_low + j_high + i_low + i_high + k_low + k_high - 6.0 * mid
                    value = (
                        mid - flow[0, j, r, here] * (j_high - j_low) - flow[1, j, r, here] * (i_high - i_low)
                        - flow[2, j, r, here] * (k_high - k_low) + SMOOTH * spread
                    )
                    if t == STEPS - 1:
                        out[j, r, here] = value
                    else:
                        field[t + 1, j + 1, r + 1, at] = value
            return 0

        lax.fori_loop(0, width, row, 0)

    loads[0].wait()
    loads[1].wait()

    def first_pack(c, _):
        pack(0, c)
        return 0

    lax.fori_loop(0, chunks, first_pack, 0)
    pl.semaphore_wait(barrier, targets)

    def first_down(c, _):
        send_down(0, c)
        return 0

    south_copy(0, 0).start()
    lax.fori_loop(0, chunks, first_down, 0)
    each(has_west, has_east, lambda side: east_copy(0, side).start())
    for c in range(1, lead):
        south_copy(0, c).start()
    for copy in loads[2:]:
        copy.wait()

    for t in range(STEPS):
        def chunk(c, _, t=t):
            each(has_up, has_down, lambda side: down_copy(t, c, 1 - side).wait_recv())
            for side, cond in ((0, has_west), (1, has_east)):
                @pl.when(jnp.logical_and(cond, c == side))
                def _(side=side):
                    east_copy(t, 1 - side).wait_recv()

            unpack(t, c)
            advance(t, c, rest_j, nj - 1)

            if t < STEPS - 1:
                @pl.when(c > 0)
                def _():
                    send_down(t + 1, c - 1)

                for side, cond in ((0, has_west), (1, has_east)):
                    @pl.when(jnp.logical_and(cond, c == side + 1))
                    def _(side=side):
                        east_copy(t + 1, side).start()

            if t > 0:
                @pl.when(c == 0)
                def _():
                    send_down(t, chunks - 1)

            late = 2
            if t < STEPS - 1:
                @pl.when(c >= late)
                def _():
                    hand_on(t + 1, c - late)

            if t > 0:
                @pl.when(c < late)
                def _():
                    hand_on(t, c + chunks - late)
            else:
                @pl.when(c == 0)
                def _():
                    for n in range(chunks):
                        hand_on(0, jnp.int32(n))

            south_copy(t, c).wait_recv()

            @pl.when(c + lead < chunks)
            def _():
                south_copy(t, c + lead).start()

            if t < STEPS - 1:
                @pl.when(c + lead >= chunks)
                def _():
                    south_copy(t + 1, c + lead - chunks).start()

            advance(t, c, my_j, 1)
            if t < STEPS - 1:
                pack(t + 1, c)
            return 0

        lax.fori_loop(0, chunks, chunk, 0)

    def finish(c, _):
        for t in range(STEPS):
            south_copy(t, c).wait_send()
            each(has_up, has_down, lambda side: down_copy(t, c, side).wait_send())
        return 0

    lax.fori_loop(0, chunks, finish, 0)
    for t in range(STEPS):
        each(has_west, has_east, lambda side: east_copy(t, side).wait_send())
        if relays:
            @pl.when(is_relay)
            def _():
                for q in range(rounds):
                    hand_on_copy(t, q, 0).wait_send()


def store_kernel(pieces, held, out, sem):
    step = held.shape[0] // pieces
    copies = [
        pltpu.make_async_copy(held.at[pl.ds(p * step, step)], out.at[pl.ds(p * step, step)], sem.at[p])
        for p in range(pieces)
    ]
    for copy in copies:
        copy.start()
    for copy in copies:
        copy.wait()


def solution(mesh, width=8, lead=2):
    sizes = tuple(mesh.shape[a] for a in ("south", "east", "down"))

    def per_device(density, flow_j, flow_i, flow_k):
        nj, ni, nk, ns = density.shape
        chunks = ni // width
        rounds = max(chunks // (sizes[2] // 2), 1)
        dma = pltpu.SemaphoreType.DMA
        held = pl.pallas_call(
            functools.partial(kernel, sizes, width, lead),
            out_shape=pltpu.VMEM(density.shape, density.dtype),
            in_specs=[pl.BlockSpec(memory_space=pl.ANY)] * 4,
            out_specs=pl.BlockSpec(memory_space=pltpu.VMEM),
            scratch_shapes=[
                pltpu.VMEM((STEPS, nj + 2, ni + 2, nk + 2 * PAD, ns), jnp.float32),
                pltpu.VMEM((3, nj, ni, nk, ns), jnp.float32),
                pltpu.VMEM((STEPS, 2, chunks, width * nj, ns), jnp.float32),
                pltpu.VMEM((STEPS, 2, chunks, width * nj, ns), jnp.float32),
                pltpu.VMEM((STEPS, rounds, width * nj, ns), jnp.float32),
                dma((5,)),
                dma((STEPS, chunks)),
                dma((STEPS, chunks)),
                dma((STEPS, 2)),
                dma((STEPS, 2)),
                dma((STEPS, chunks, 2)),
                dma((STEPS, chunks, 2)),
                dma((STEPS, rounds)),
                dma((STEPS, rounds)),
            ],
            compiler_params=pltpu.CompilerParams(
                collective_id=0, has_side_effects=True, vmem_limit_bytes=48 * 1024 * 1024
            ),
            name="advect",
        )(density, flow_j, flow_i, flow_k)
        return pl.pallas_call(
            functools.partial(store_kernel, nj),
            out_shape=jax.ShapeDtypeStruct(density.shape, density.dtype),
            in_specs=[pl.BlockSpec(memory_space=pltpu.VMEM)],
            out_specs=pl.BlockSpec(memory_space=pl.ANY),
            scratch_shapes=[dma((nj,))],
            compiler_params=pltpu.CompilerParams(vmem_limit_bytes=8 * 1024 * 1024),
            name="store",
        )(held)

    spec = P(("ens", "south"), "east", "down", None)
    return jax.shard_map(per_device, mesh=mesh, in_specs=(spec,) * 4, out_specs=spec, check_vma=False)
```

```python
import functools

import jax
import jax.numpy as jnp
from jax import lax
from jax.experimental import pallas as pl
from jax.experimental.pallas import tpu as pltpu
from jax.sharding import PartitionSpec as P

STEPS = 3
SMOOTH = 0.05
PAD = 8


def kernel(
    sizes, width, lead, den, fj, fi, fk, out, field, flow, k_send, k_recv, k_relay,
    load_sem, south_send, south_recv, east_send, east_recv, down_send, down_recv, relay_send, relay_recv, pair_sem,
):
    _, n_east, n_down = sizes
    nj, ni, nk, ns = den.shape
    chunks = ni // width
    half = n_down // 2
    relays = chunks % half == 0
    rounds = chunks // half
    south, east, down = (lax.axis_index(a) for a in ("south", "east", "down"))
    has_west, has_east = east > 0, east < n_east - 1
    has_up, has_down = down > 0, down < n_down - 1
    inner_k = pl.ds(PAD, nk)
    my_j = jnp.where(south == 0, nj - 1, 0)
    their_j = jnp.where(south == 0, 0, nj + 1)
    rest_j = jnp.where(south == 0, 0, 1)

    def to(axis, index):
        return dict(device_id={axis: index}, device_id_type=pl.DeviceIdType.MESH)

    def each(cond_low, cond_high, fn):
        for side, cond in ((0, cond_low), (1, cond_high)):
            @pl.when(cond)
            def _(side=side):
                fn(side)

    def row_of(c):
        return width * jnp.where(c == 0, 0, jnp.where(c == 1, chunks - 1, c - 1))

    lower = down < half
    at_seam = jnp.logical_or(down == half - 1, down == half)
    mine = lax.rem(down, half)
    own_end = jnp.where(lower, half - 1, half)
    far_end = jnp.where(lower, half, half - 1)
    far_base = jnp.where(lower, half, 0)
    own_base = jnp.where(lower, 0, half)
    own_side = jnp.where(lower, 0, 1)
    is_relay = jnp.logical_not(at_seam)

    even = lax.rem(east, 2) == 0
    hub = east - lax.rem(east, 2)
    barrier = pltpu.get_barrier_semaphore()

    def hello(cond, index, **others):
        @pl.when(cond)
        def _():
            pl.semaphore_signal(
                barrier, inc=1, device_id={"east": index, **others}, device_id_type=pl.DeviceIdType.MESH)

    always = down >= 0
    near_up = jnp.logical_and(has_up, jnp.logical_not(jnp.logical_and(at_seam, jnp.logical_not(lower))))
    near_down = jnp.logical_and(has_down, jnp.logical_not(jnp.logical_and(at_seam, lower)))
    hello(always, hub, south=1 - south)
    hello(jnp.logical_and(even, has_west), east - 2)
    hello(jnp.logical_not(even), east - 1)
    hello(jnp.logical_and(jnp.logical_not(even), has_east), east + 1)
    hello(near_up, hub, down=down - 1)
    hello(near_down, hub, down=down + 1)
    if relays:
        hello(is_relay, hub, down=own_end)
        for m in range(half):
            hello(at_seam, hub + 1, down=far_base + m)
    else:
        hello(at_seam, hub + 1, down=far_end)

    loads = [
        pltpu.make_async_copy(den.at[my_j], field.at[0, my_j + 1, pl.ds(1, ni), inner_k], load_sem.at[0]),
        pltpu.make_async_copy(
            den.at[pl.ds(rest_j, nj - 1)], field.at[0, pl.ds(rest_j + 1, nj - 1), pl.ds(1, ni), inner_k], load_sem.at[1]),
    ]
    for x, src in enumerate((fj, fi, fk)):
        loads.append(pltpu.make_async_copy(src, flow.at[x], load_sem.at[x + 2]))
    for copy in loads:
        copy.start()

    def south_copy(t, c):
        rows = pl.ds(row_of(c) + 1, width)
        return pltpu.make_async_remote_copy(
            src_ref=field.at[t, my_j + 1, rows, inner_k], dst_ref=field.at[t, their_j, rows, inner_k],
            send_sem=south_send.at[t, c], recv_sem=south_recv.at[t, c], **to("south", 1 - south))

    def east_copy(t, side):
        r, dst, other = (1, ni + 1, east - 1) if side == 0 else (ni, 0, east + 1)
        return pltpu.make_async_remote_copy(
            src_ref=field.at[t, pl.ds(1, nj), r, inner_k], dst_ref=field.at[t, pl.ds(1, nj), dst, inner_k],
            send_sem=east_send.at[t, side], recv_sem=east_recv.at[t, 1 - side], **to("east", other))

    def down_copy(t, c, side):
        other = down - 1 if side == 0 else down + 1
        return pltpu.make_async_remote_copy(
            src_ref=k_send.at[t, side, c], dst_ref=k_recv.at[t, 1 - side, c],
            send_sem=down_send.at[t, c, side], recv_sem=down_recv.at[t, c, 1 - side], **to("down", other))

    def detour_copy(t, c, side):
        return pltpu.make_async_remote_copy(
            src_ref=k_send.at[t, side, c], dst_ref=k_relay.at[t, c // half],
            send_sem=down_send.at[t, c, side], recv_sem=relay_recv.at[t, c // half],
            **to("down", own_base + lax.rem(c, half)))

    def hand_on_copy(t, q, side):
        return pltpu.make_async_remote_copy(
            src_ref=k_relay.at[t, q], dst_ref=k_recv.at[t, side, mine + q * half],
            send_sem=relay_send.at[t, q], recv_sem=down_recv.at[t, mine + q * half, side], **to("down", far_end))

    def send_down(t, c, near=None):
        def one(side):
            crosses = down == (half if side == 0 else half - 1)
            around = jnp.logical_and(crosses, own_base + lax.rem(c, half) != own_end) if relays else down < 0
            far = jnp.logical_and(crosses, jnp.logical_not(around))
            straight = jnp.logical_not(around)
            if near is not None:
                straight = far if not near else jnp.logical_not(crosses)

            if near is not False:
                @pl.when(around)
                def _():
                    detour_copy(t, c, side).start()

            @pl.when(straight)
            def _():
                down_copy(t, c, side).start()

        each(has_up, has_down, one)

    def hand_on(t, n):
        if not relays:
            return

        @pl.when(jnp.logical_and(is_relay, lax.rem(n, half) == mine))
        def _():
            q = n // half
            pltpu.make_async_remote_copy(
                src_ref=k_relay.at[t, q], dst_ref=k_relay.at[t, q],
                send_sem=relay_send.at[t, q], recv_sem=relay_recv.at[t, q], **to("down", far_end)).wait_recv()
            hand_on_copy(t, q, own_side).start()

    def ends(t, c, w):
        r = row_of(c) + w + 1
        for j in range(nj):
            yield j + 1, r, pl.ds(w * nj + j, 1)

    def pack(t, c):
        def row(w, _):
            for j, r, at in ends(t, c, w):
                k_send[t, 0, c, at] = field[t, j, r, pl.ds(PAD, 1)]
                k_send[t, 1, c, at] = field[t, j, r, pl.ds(PAD + nk - 1, 1)]
            return 0

        lax.fori_loop(0, width, row, 0)

    def unpack(t, c):
        def row(w, _):
            for j, r, at in ends(t, c, w):
                field[t, j, r, pl.ds(PAD - 1, 1)] = k_recv[t, 0, c, at]
                field[t, j, r, pl.ds(PAD + nk, 1)] = k_recv[t, 1, c, at]
            return 0

        lax.fori_loop(0, width, row, 0)

    def advance(t, c, first, count):
        def row(w, _):
            r = row_of(c) + w
            for b in range(nk // 8):
                at, here = pl.ds(PAD + 8 * b, 8), pl.ds(8 * b, 8)
                column = [field[t, first + p, r + 1, at] for p in range(count + 2)]
                for p in range(count):
                    j = first + p
                    mid, j_low, j_high = column[p + 1], column[p], column[p + 2]
                    i_low, i_high = field[t, j + 1, r, at], field[t, j + 1, r + 2, at]
                    k_low = field[t, j + 1, r + 1, pl.ds(PAD + 8 * b - 1, 8)]
                    k_high = field[t, j + 1, r + 1, pl.ds(PAD + 8 * b + 1, 8)]
                    spread = j_low + j_high + i_low + i_high + k_low + k_high - 6.0 * mid
                    value = (
                        mid - flow[0, j, r, here] * (j_high - j_low) - flow[1, j, r, here] * (i_high - i_low)
                        - flow[2, j, r, here] * (k_high - k_low) + SMOOTH * spread
                    )
                    if t == STEPS - 1:
                        out[j, r, here] = value
                    else:
                        field[t + 1, j + 1, r + 1, at] = value
            return 0

        lax.fori_loop(0, width, row, 0)

    loads[0].wait()

    @pl.when(even)
    def _():
        one = lambda cond, n: jnp.where(cond, n, 0)
        pl.semaphore_wait(
            barrier, 3 + one(east > 0, 1) + one(east < n_east - 2, 1) + one(near_up, 2) + one(near_down, 2)
            + (one(at_seam, 2 * (half - 1)) if relays else 0))
        pl.semaphore_signal(pair_sem.at[0], inc=1, **to("east", east + 1))

    @pl.when(jnp.logical_not(even))
    def _():
        pl.semaphore_wait(pair_sem.at[0], 1)

    south_copy(0, 0).start()
    loads[1].wait()
    each(has_west, has_east, lambda side: east_copy(0, side).start())

    def first_pack(c, _):
        pack(0, c)
        return 0

    lax.fori_loop(0, chunks, first_pack, 0)

    def first_down(c, _):
        send_down(0, c, True)
        return 0

    lax.fori_loop(0, chunks, first_down, 0)

    outside_j = jnp.where(south == 0, 0, nj + 1)

    def clear(n, _):
        for t in range(STEPS):
            field[t, outside_j, n + 1, inner_k] = jnp.zeros((nk, ns), jnp.float32)
        return 0

    lax.fori_loop(0, ni, clear, 0)
    for edge, at in ((jnp.logical_not(has_west), 0), (jnp.logical_not(has_east), ni + 1)):
        @pl.when(edge)
        def _(at=at):
            for t in range(STEPS):
                for j in range(nj):
                    field[t, j + 1, at, inner_k] = jnp.zeros((nk, ns), jnp.float32)
    for edge, side in ((jnp.logical_not(has_up), 0), (jnp.logical_not(has_down), 1)):
        @pl.when(edge)
        def _(side=side):
            for t in range(STEPS):
                for c in range(chunks):
                    k_recv[t, side, c] = jnp.zeros(k_recv.shape[3:], jnp.float32)

    @pl.when(jnp.logical_not(even))
    def _():
        pl.semaphore_wait(barrier, 2)
        pl.semaphore_signal(pair_sem.at[1], inc=1, **to("east", east - 1))

    @pl.when(even)
    def _():
        pl.semaphore_wait(pair_sem.at[1], 1)

    def first_far(c, _):
        send_down(0, c, False)
        return 0

    lax.fori_loop(0, chunks, first_far, 0)
    for n in range(chunks):
        hand_on(0, jnp.int32(n))
    for c in range(1, lead):
        south_copy(0, c).start()
    for copy in loads[2:]:
        copy.wait()

    def arrive(t, c):
        south_copy(t, c).wait_recv()
        if t < STEPS - 1:
            @pl.when(c > 0)
            def _():
                hand_on(t + 1, c - 1)

        if t > 0:
            @pl.when(c == 0)
            def _():
                hand_on(t, c + chunks - 1)

        @pl.when(c + lead < chunks)
        def _():
            south_copy(t, c + lead).start()

        if t < STEPS - 1:
            @pl.when(c + lead >= chunks)
            def _():
                south_copy(t + 1, c + lead - chunks).start()

    def surround(t, c):
        each(has_up, has_down, lambda side: down_copy(t, c, 1 - side).wait_recv())
        for side, cond in ((0, has_west), (1, has_east)):
            @pl.when(jnp.logical_and(cond, c == side))
            def _(side=side):
                east_copy(t, 1 - side).wait_recv()

        unpack(t, c)

    def sent(t, c):
        south_copy(t, c).wait_send()
        each(has_up, has_down, lambda side: down_copy(t, c, side).wait_send())

    for t in range(STEPS - 1):
        def chunk(c, _, t=t):
            arrive(t, c)
            surround(t, c)
            advance(t, c, 0, nj)
            pack(t + 1, c)
            send_down(t + 1, c)
            for side, cond in ((0, has_west), (1, has_east)):
                @pl.when(jnp.logical_and(cond, c == side))
                def _(side=side):
                    east_copy(t + 1, side).start()
            return 0

        lax.fori_loop(0, chunks, chunk, 0)

    t = STEPS - 1

    def last_chunk(c, _):
        early = c + lead < chunks

        @pl.when(early)
        def _():
            arrive(t, c)

        surround(t, c)
        advance(t, c, rest_j, nj - 1)

        @pl.when(c == chunks - 1)
        def _():
            def finish(n, _):
                for s in range(STEPS - 1):
                    sent(s, n)
                each(has_up, has_down, lambda side: down_copy(t, n, side).wait_send())
                return 0

            lax.fori_loop(0, chunks, finish, 0)
            for s in range(STEPS):
                each(has_west, has_east, lambda side: east_copy(s, side).wait_send())
                if relays:
                    @pl.when(is_relay)
                    def _():
                        for q in range(rounds):
                            hand_on_copy(s, q, 0).wait_send()

        @pl.when(jnp.logical_not(early))
        def _():
            south_copy(t, c).wait_recv()

        advance(t, c, my_j, 1)
        return 0

    lax.fori_loop(0, chunks, last_chunk, 0)
    for c in range(chunks):
        south_copy(t, c).wait_send()


def store_kernel(pieces, held, out, sem):
    nj, ni = held.shape[:2]
    step = nj * ni // pieces
    copies = [
        pltpu.make_async_copy(
            held.at[p * step // ni, pl.ds(p * step % ni, step)], out.at[p * step // ni, pl.ds(p * step % ni, step)], sem.at[p])
        for p in range(pieces)
    ]
    for copy in copies:
        copy.start()
    for copy in copies:
        copy.wait()


def solution(mesh, width=8, lead=2):
    sizes = tuple(mesh.shape[a] for a in ("south", "east", "down"))

    def per_device(density, flow_j, flow_i, flow_k):
        nj, ni, nk, ns = density.shape
        chunks = ni // width
        rounds = max(chunks // (sizes[2] // 2), 1)
        dma = pltpu.SemaphoreType.DMA
        held = pl.pallas_call(
            functools.partial(kernel, sizes, width, lead),
            out_shape=pltpu.VMEM(density.shape, density.dtype),
            in_specs=[pl.BlockSpec(memory_space=pl.ANY)] * 4,
            out_specs=pl.BlockSpec(memory_space=pltpu.VMEM),
            scratch_shapes=[
                pltpu.VMEM((STEPS, nj + 2, ni + 2, nk + 2 * PAD, ns), jnp.float32),
                pltpu.VMEM((3, nj, ni, nk, ns), jnp.float32),
                pltpu.VMEM((STEPS, 2, chunks, width * nj, ns), jnp.float32),
                pltpu.VMEM((STEPS, 2, chunks, width * nj, ns), jnp.float32),
                pltpu.VMEM((STEPS, rounds, width * nj, ns), jnp.float32),
                dma((5,)),
                dma((STEPS, chunks)),
                dma((STEPS, chunks)),
                dma((STEPS, 2)),
                dma((STEPS, 2)),
                dma((STEPS, chunks, 2)),
                dma((STEPS, chunks, 2)),
                dma((STEPS, rounds)),
                dma((STEPS, rounds)),
                pltpu.SemaphoreType.REGULAR((2,)),
            ],
            compiler_params=pltpu.CompilerParams(
                collective_id=0, has_side_effects=True, vmem_limit_bytes=48 * 1024 * 1024
            ),
            name="advect",
        )(density, flow_j, flow_i, flow_k)
        return pl.pallas_call(
            functools.partial(store_kernel, nj),
            out_shape=jax.ShapeDtypeStruct(density.shape, density.dtype),
            in_specs=[pl.BlockSpec(memory_space=pltpu.VMEM)],
            out_specs=pl.BlockSpec(memory_space=pl.ANY),
            scratch_shapes=[dma((nj,))],
            compiler_params=pltpu.CompilerParams(vmem_limit_bytes=8 * 1024 * 1024),
            name="store",
        )(held)

    spec = P(("ens", "south"), "east", "down", None)
    return jax.shard_map(per_device, mesh=mesh, in_specs=(spec,) * 4, out_specs=spec, check_vma=False)
```

```python
import functools

import jax
import jax.numpy as jnp
from jax import lax
from jax.experimental import pallas as pl
from jax.experimental.pallas import tpu as pltpu
from jax.sharding import PartitionSpec as P

STEPS = 3
SMOOTH = 0.05
PAD = 8


def kernel(
    sizes, width, lead, den, fj, fi, fk, out, field, flow, k_send, k_recv, k_relay,
    load_sem, south_send, south_recv, east_send, east_recv, down_send, down_recv, relay_send, relay_recv, pair_sem,
):
    _, n_east, n_down = sizes
    nj, ni, nk, ns = den.shape
    chunks = ni // width
    half = n_down // 2
    assert chunks % half == 0
    rounds = chunks // half
    south, east, down = (lax.axis_index(a) for a in ("south", "east", "down"))
    has_west, has_east = east > 0, east < n_east - 1
    has_up, has_down = down > 0, down < n_down - 1
    inner_k = pl.ds(PAD, nk)
    my_j = jnp.where(south == 0, nj - 1, 0)
    their_j = jnp.where(south == 0, 0, nj + 1)
    rest_j = jnp.where(south == 0, 0, 1)

    def to(axis, index):
        return dict(device_id={axis: index}, device_id_type=pl.DeviceIdType.MESH)

    def each(cond_low, cond_high, fn):
        for side, cond in ((0, cond_low), (1, cond_high)):
            @pl.when(cond)
            def _(side=side):
                fn(side)

    def row_of(c):
        return width * jnp.where(c == 0, 0, jnp.where(c == 1, chunks - 1, c - 1))

    lower = down < half
    at_seam = jnp.logical_or(down == half - 1, down == half)
    mine = lax.rem(down, half)
    own_end = jnp.where(lower, half - 1, half)
    far_end = jnp.where(lower, half, half - 1)
    far_base = jnp.where(lower, half, 0)
    own_base = jnp.where(lower, 0, half)
    own_side = jnp.where(lower, 0, 1)
    is_relay = jnp.logical_not(at_seam)

    loads = [
        pltpu.make_async_copy(den.at[my_j], field.at[0, my_j + 1, pl.ds(1, ni), inner_k], load_sem.at[0]),
        pltpu.make_async_copy(
            den.at[pl.ds(rest_j, nj - 1)], field.at[0, pl.ds(rest_j + 1, nj - 1), pl.ds(1, ni), inner_k], load_sem.at[1]),
    ]
    for x, src in enumerate((fj, fi, fk)):
        loads.append(pltpu.make_async_copy(src, flow.at[x], load_sem.at[x + 2]))
    even = lax.rem(east, 2) == 0
    odd = jnp.logical_not(even)
    hub = east - lax.rem(east, 2)
    barrier = pltpu.get_barrier_semaphore()

    def hello(cond, index, **others):
        @pl.when(cond)
        def _():
            pl.semaphore_signal(
                barrier, inc=1, device_id={"east": index, **others}, device_id_type=pl.DeviceIdType.MESH)

    near_up = jnp.logical_and(has_up, down != half)
    near_down = jnp.logical_and(has_down, down != half - 1)
    hello(down >= 0, hub, south=1 - south)
    hello(odd, hub)
    loads[0].start()
    hello(jnp.logical_and(even, has_west), east - 1, south=0)
    hello(jnp.logical_and(odd, has_east), east + 2, south=0)
    hello(near_up, hub + 1, south=0, down=down - 1)
    hello(near_down, hub + 1, south=0, down=down + 1)
    hello(is_relay, hub + 1, south=0, down=own_end)
    for m in range(half):
        hello(at_seam, hub + 1, south=1, down=far_base + m)

    def one(cond, n):
        return jnp.where(cond, n, 0)

    def learn(n, who, count):
        taker = jnp.logical_and(odd, south == who)

        @pl.when(taker)
        def _():
            pl.semaphore_wait(barrier, count)
            for s, e in ((who, hub), (1 - who, hub), (1 - who, hub + 1)):
                pl.semaphore_signal(
                    pair_sem.at[n], inc=1, device_id={"south": s, "east": e}, device_id_type=pl.DeviceIdType.MESH)

        @pl.when(jnp.logical_not(taker))
        def _():
            pl.semaphore_wait(pair_sem.at[n], 1)

    for copy in loads[1:]:
        copy.start()

    def south_copy(t, c):
        rows = pl.ds(row_of(c) + 1, width)
        return pltpu.make_async_remote_copy(
            src_ref=field.at[t, my_j + 1, rows, inner_k], dst_ref=field.at[t, their_j, rows, inner_k],
            send_sem=south_send.at[t, c], recv_sem=south_recv.at[t, c], **to("south", 1 - south))

    def east_copy(t, side):
        r, dst, other = (1, ni + 1, east - 1) if side == 0 else (ni, 0, east + 1)
        return pltpu.make_async_remote_copy(
            src_ref=field.at[t, pl.ds(1, nj), r, inner_k], dst_ref=field.at[t, pl.ds(1, nj), dst, inner_k],
            send_sem=east_send.at[t, side], recv_sem=east_recv.at[t, 1 - side], **to("east", other))

    def down_copy(t, c, side):
        other = down - 1 if side == 0 else down + 1
        return pltpu.make_async_remote_copy(
            src_ref=k_send.at[t, side, c], dst_ref=k_recv.at[t, 1 - side, c],
            send_sem=down_send.at[t, c, side], recv_sem=down_recv.at[t, c, 1 - side], **to("down", other))

    def detour_copy(t, c, side):
        return pltpu.make_async_remote_copy(
            src_ref=k_send.at[t, side, c], dst_ref=k_relay.at[t, c // half],
            send_sem=down_send.at[t, c, side], recv_sem=relay_recv.at[t, c // half],
            **to("down", own_base + lax.rem(c, half)))

    def hand_on_copy(t, q, side):
        return pltpu.make_async_remote_copy(
            src_ref=k_relay.at[t, q], dst_ref=k_recv.at[t, side, mine + q * half],
            send_sem=relay_send.at[t, q], recv_sem=down_recv.at[t, mine + q * half, side], **to("down", far_end))

    def send_down(t, c, near=None):
        def one(side):
            crosses = down == (half if side == 0 else half - 1)
            around = jnp.logical_and(crosses, own_base + lax.rem(c, half) != own_end)
            far = jnp.logical_and(crosses, jnp.logical_not(around))
            straight = jnp.logical_not(around)
            if near is not None:
                straight = far if not near else jnp.logical_not(crosses)

            if near is not False:
                @pl.when(around)
                def _():
                    detour_copy(t, c, side).start()

            @pl.when(straight)
            def _():
                down_copy(t, c, side).start()

        each(has_up, has_down, one)

    def hand_on(t, n):
        @pl.when(jnp.logical_and(is_relay, lax.rem(n, half) == mine))
        def _():
            q = n // half
            pltpu.make_async_remote_copy(
                src_ref=k_relay.at[t, q], dst_ref=k_relay.at[t, q],
                send_sem=relay_send.at[t, q], recv_sem=relay_recv.at[t, q], **to("down", far_end)).wait_recv()
            hand_on_copy(t, q, own_side).start()

    def ends(t, c, w):
        r = row_of(c) + w + 1
        for j in range(nj):
            yield j + 1, r, pl.ds(w * nj + j, 1)

    def pack(t, c):
        def row(w, _):
            for j, r, at in ends(t, c, w):
                k_send[t, 0, c, at] = field[t, j, r, pl.ds(PAD, 1)]
                k_send[t, 1, c, at] = field[t, j, r, pl.ds(PAD + nk - 1, 1)]
            return 0

        lax.fori_loop(0, width, row, 0)

    def unpack(t, c):
        def row(w, _):
            for j, r, at in ends(t, c, w):
                field[t, j, r, pl.ds(PAD - 1, 1)] = k_recv[t, 0, c, at]
                field[t, j, r, pl.ds(PAD + nk, 1)] = k_recv[t, 1, c, at]
            return 0

        lax.fori_loop(0, width, row, 0)

    def advance(t, c, first, count):
        def row(w, _):
            r = row_of(c) + w
            for b in range(nk // 8):
                at, here = pl.ds(PAD + 8 * b, 8), pl.ds(8 * b, 8)
                column = [field[t, first + p, r + 1, at] for p in range(count + 2)]
                for p in range(count):
                    j = first + p
                    mid, j_low, j_high = column[p + 1], column[p], column[p + 2]
                    i_low, i_high = field[t, j + 1, r, at], field[t, j + 1, r + 2, at]
                    k_low = field[t, j + 1, r + 1, pl.ds(PAD + 8 * b - 1, 8)]
                    k_high = field[t, j + 1, r + 1, pl.ds(PAD + 8 * b + 1, 8)]
                    spread = j_low + j_high + i_low + i_high + k_low + k_high - 6.0 * mid
                    value = (
                        mid - flow[0, j, r, here] * (j_high - j_low) - flow[1, j, r, here] * (i_high - i_low)
                        - flow[2, j, r, here] * (k_high - k_low) + SMOOTH * spread
                    )
                    if t == STEPS - 1:
                        out[j, r, here] = value
                    else:
                        field[t + 1, j + 1, r + 1, at] = value
            return 0

        lax.fori_loop(0, width, row, 0, unroll=2)

    loads[0].wait()

    @pl.when(even)
    def _():
        pl.semaphore_wait(barrier, 3)
        pl.semaphore_signal(pair_sem.at[0], inc=1, **to("east", east + 1))

    @pl.when(odd)
    def _():
        pl.semaphore_wait(pair_sem.at[0], 1)

    south_copy(0, 0).start()
    loads[1].wait()

    def first_pack(c, _):
        pack(0, c)
        return 0

    lax.fori_loop(0, chunks, first_pack, 0)
    learn(1, 0, one(hub > 0, 2) + one(hub + 2 < n_east, 2) + one(near_up, 4) + one(near_down, 4)
          + one(at_seam, 4 * (half - 1)))
    each(has_west, has_east, lambda side: east_copy(0, side).start())

    def first_down(c, _):
        send_down(0, c, True)
        return 0

    lax.fori_loop(0, chunks, first_down, 0)

    outside_j = jnp.where(south == 0, 0, nj + 1)

    def clear(n, _):
        for t in range(STEPS):
            field[t, outside_j, n + 1, inner_k] = jnp.zeros((nk, ns), jnp.float32)
        return 0

    lax.fori_loop(0, ni, clear, 0)
    for edge, at in ((jnp.logical_not(has_west), 0), (jnp.logical_not(has_east), ni + 1)):
        @pl.when(edge)
        def _(at=at):
            for t in range(STEPS):
                for j in range(nj):
                    field[t, j + 1, at, inner_k] = jnp.zeros((nk, ns), jnp.float32)
    for edge, side in ((jnp.logical_not(has_up), 0), (jnp.logical_not(has_down), 1)):
        @pl.when(edge)
        def _(side=side):
            for t in range(STEPS):
                for c in range(chunks):
                    k_recv[t, side, c] = jnp.zeros(k_recv.shape[3:], jnp.float32)

    learn(2, 1, 4)

    def first_far(c, _):
        send_down(0, c, False)
        return 0

    lax.fori_loop(0, chunks, first_far, 0)
    for n in range(chunks):
        hand_on(0, jnp.int32(n))
    for c in range(1, lead):
        south_copy(0, c).start()
    for copy in loads[2:]:
        copy.wait()

    def pass_on(t, c):
        if t < STEPS - 1:
            @pl.when(c > 0)
            def _():
                hand_on(t + 1, c - 1)

        if t > 0:
            @pl.when(c == 0)
            def _():
                hand_on(t, c + chunks - 1)

    def arrive(t, c):
        south_copy(t, c).wait_recv()
        pass_on(t, c)

        @pl.when(c + lead < chunks)
        def _():
            south_copy(t, c + lead).start()

        if t < STEPS - 1:
            @pl.when(c + lead >= chunks)
            def _():
                south_copy(t + 1, c + lead - chunks).start()

    def surround(t, c):
        each(has_up, has_down, lambda side: down_copy(t, c, 1 - side).wait_recv())
        for side, cond in ((0, has_west), (1, has_east)):
            @pl.when(jnp.logical_and(cond, c == side))
            def _(side=side):
                east_copy(t, 1 - side).wait_recv()

        unpack(t, c)

    def sent(t, c):
        south_copy(t, c).wait_send()
        each(has_up, has_down, lambda side: down_copy(t, c, side).wait_send())

    for t in range(STEPS - 1):
        def chunk(c, _, t=t):
            arrive(t, c)
            surround(t, c)
            advance(t, c, 0, nj)
            pack(t + 1, c)
            send_down(t + 1, c)
            for side, cond in ((0, has_west), (1, has_east)):
                @pl.when(jnp.logical_and(cond, c == side))
                def _(side=side):
                    east_copy(t + 1, side).start()
            return 0

        lax.fori_loop(0, chunks, chunk, 0)

    t = STEPS - 1

    def last_chunk(c, _):
        early = c + lead < chunks

        @pl.when(early)
        def _():
            arrive(t, c)

        surround(t, c)
        advance(t, c, rest_j, nj - 1)

        @pl.when(c == chunks - 1)
        def _():
            def finish(n, _):
                for s in range(STEPS - 1):
                    sent(s, n)
                each(has_up, has_down, lambda side: down_copy(t, n, side).wait_send())
                return 0

            lax.fori_loop(0, chunks, finish, 0)
            for s in range(STEPS):
                each(has_west, has_east, lambda side: east_copy(s, side).wait_send())

                @pl.when(is_relay)
                def _(s=s):
                    for q in range(rounds):
                        hand_on_copy(s, q, 0).wait_send()

        @pl.when(jnp.logical_not(early))
        def _():
            south_copy(t, c).wait_recv()

        advance(t, c, my_j, 1)
        return 0

    lax.fori_loop(0, chunks, last_chunk, 0)
    for c in range(chunks):
        south_copy(t, c).wait_send()


def store_kernel(pieces, held, out, sem):
    nj, ni = held.shape[:2]
    step = nj * ni // pieces
    copies = [
        pltpu.make_async_copy(
            held.at[p * step // ni, pl.ds(p * step % ni, step)], out.at[p * step // ni, pl.ds(p * step % ni, step)], sem.at[p])
        for p in range(pieces)
    ]
    for copy in copies:
        copy.start()
    for copy in copies:
        copy.wait()


def solution(mesh, width=8, lead=2):
    sizes = tuple(mesh.shape[a] for a in ("south", "east", "down"))

    def per_device(density, flow_j, flow_i, flow_k):
        nj, ni, nk, ns = density.shape
        chunks = ni // width
        rounds = max(chunks // (sizes[2] // 2), 1)
        dma = pltpu.SemaphoreType.DMA
        held = pl.pallas_call(
            functools.partial(kernel, sizes, width, lead),
            out_shape=pltpu.VMEM(density.shape, density.dtype),
            in_specs=[pl.BlockSpec(memory_space=pl.ANY)] * 4,
            out_specs=pl.BlockSpec(memory_space=pltpu.VMEM),
            scratch_shapes=[
                pltpu.VMEM((STEPS, nj + 2, ni + 2, nk + 2 * PAD, ns), jnp.float32),
                pltpu.VMEM((3, nj, ni, nk, ns), jnp.float32),
                pltpu.VMEM((STEPS, 2, chunks, width * nj, ns), jnp.float32),
                pltpu.VMEM((STEPS, 2, chunks, width * nj, ns), jnp.float32),
                pltpu.VMEM((STEPS, rounds, width * nj, ns), jnp.float32),
                dma((5,)),
                dma((STEPS, chunks)),
                dma((STEPS, chunks)),
                dma((STEPS, 2)),
                dma((STEPS, 2)),
                dma((STEPS, chunks, 2)),
                dma((STEPS, chunks, 2)),
                dma((STEPS, rounds)),
                dma((STEPS, rounds)),
                pltpu.SemaphoreType.REGULAR((3,)),
            ],
            compiler_params=pltpu.CompilerParams(
                collective_id=0, has_side_effects=True, vmem_limit_bytes=48 * 1024 * 1024
            ),
            name="advect",
        )(density, flow_j, flow_i, flow_k)
        return pl.pallas_call(
            functools.partial(store_kernel, nj),
            out_shape=jax.ShapeDtypeStruct(density.shape, density.dtype),
            in_specs=[pl.BlockSpec(memory_space=pltpu.VMEM)],
            out_specs=pl.BlockSpec(memory_space=pl.ANY),
            scratch_shapes=[dma((nj,))],
            compiler_params=pltpu.CompilerParams(vmem_limit_bytes=8 * 1024 * 1024),
            name="store",
        )(held)

    spec = P(("ens", "south"), "east", "down", None)
    return jax.shard_map(per_device, mesh=mesh, in_specs=(spec,) * 4, out_specs=spec, check_vma=False)
```

```python
import functools

import jax
import jax.numpy as jnp
from jax import lax
from jax.experimental import pallas as pl
from jax.experimental.pallas import tpu as pltpu
from jax.sharding import PartitionSpec as P

STEPS = 3
SMOOTH = 0.05
PAD = 8
ROUTES = ((0, 1, 2, 3), (1, 2, 3, 1), (2, 1, 3, 2))


def kernel(
    sizes, width, lead, den, fj, fi, fk, out, field, flow, k_send, k_recv, k_relay,
    load_sem, south_send, south_recv, east_send, east_recv, down_send, down_recv, relay_send, relay_recv, pair_sem,
):
    _, n_east, n_down = sizes
    nj, ni, nk, ns = den.shape
    chunks = ni // width
    half = n_down // 2
    assert chunks == len(ROUTES[0]) == half
    south, east, down = (lax.axis_index(a) for a in ("south", "east", "down"))
    has_west, has_east = east > 0, east < n_east - 1
    has_up, has_down = down > 0, down < n_down - 1
    inner_k = pl.ds(PAD, nk)
    my_j = jnp.where(south == 0, nj - 1, 0)
    their_j = jnp.where(south == 0, 0, nj + 1)
    rest_j = jnp.where(south == 0, 0, 1)

    def to(axis, index):
        return dict(device_id={axis: index}, device_id_type=pl.DeviceIdType.MESH)

    def each(cond_low, cond_high, fn):
        for side, cond in ((0, cond_low), (1, cond_high)):
            @pl.when(cond)
            def _(side=side):
                fn(side)

    def row_of(c):
        return width * jnp.where(c == 0, 0, jnp.where(c == 1, chunks - 1, c - 1))

    lower = down < half
    at_seam = jnp.logical_or(down == half - 1, down == half)
    mine = lax.rem(down, half)
    own_end = jnp.where(lower, half - 1, half)
    far_end = jnp.where(lower, half, half - 1)
    far_base = jnp.where(lower, half, 0)
    own_base = jnp.where(lower, 0, half)
    own_side = jnp.where(lower, 0, 1)
    is_relay = jnp.logical_not(at_seam)
    def route(t, c):
        n = ROUTES[t][0]
        for x in range(1, chunks):
            n = jnp.where(c == x, ROUTES[t][x], n)
        return n


    def plane_load(n, first, count):
        return pltpu.make_async_copy(
            den.at[my_j, pl.ds(first, count)], field.at[0, my_j + 1, pl.ds(first + 1, count), inner_k], load_sem.at[n])

    loads = [
        plane_load(0, 0, width),
        plane_load(1, width, ni - width),
        pltpu.make_async_copy(
            den.at[pl.ds(rest_j, nj - 1)], field.at[0, pl.ds(rest_j + 1, nj - 1), pl.ds(1, ni), inner_k], load_sem.at[2]),
    ]
    for x, src in enumerate((fj, fi, fk)):
        loads.append(pltpu.make_async_copy(src, flow.at[x], load_sem.at[x + 3]))

    even = lax.rem(east, 2) == 0
    odd = jnp.logical_not(even)
    hub = east - lax.rem(east, 2)
    barrier = pltpu.get_barrier_semaphore()

    def hello(cond, index, **others):
        @pl.when(cond)
        def _():
            pl.semaphore_signal(
                barrier, inc=1, device_id={"east": index, **others}, device_id_type=pl.DeviceIdType.MESH)

    near_up = jnp.logical_and(has_up, down != half)
    near_down = jnp.logical_and(has_down, down != half - 1)
    loads[0].start()
    hello(down >= 0, hub, south=1 - south)
    hello(odd, hub)
    hello(jnp.logical_and(even, has_west), east - 1, south=0)
    hello(jnp.logical_and(odd, has_east), east + 2, south=0)
    hello(near_up, hub + 1, south=0, down=down - 1)
    hello(near_down, hub + 1, south=0, down=down + 1)
    hello(is_relay, hub + 1, south=0, down=own_end)
    for m in range(half):
        hello(at_seam, hub + 1, south=1, down=far_base + m)

    def one(cond, n):
        return jnp.where(cond, n, 0)

    def learn(n, who, count):
        taker = jnp.logical_and(odd, south == who)

        @pl.when(taker)
        def _():
            pl.semaphore_wait(barrier, count)
            for s, e in ((who, hub), (1 - who, hub), (1 - who, hub + 1)):
                pl.semaphore_signal(
                    pair_sem.at[n], inc=1, device_id={"south": s, "east": e}, device_id_type=pl.DeviceIdType.MESH)

        @pl.when(jnp.logical_not(taker))
        def _():
            pl.semaphore_wait(pair_sem.at[n], 1)

    for copy in loads[1:3]:
        copy.start()

    def south_copy(t, c, part=None):
        if part is None:
            rows = pl.ds(row_of(c) + 1, width)
        else:
            rows = pl.ds(row_of(c) + 1 + part * (width // 2), width // 2)
            c = chunks - 1 + part
        return pltpu.make_async_remote_copy(
            src_ref=field.at[t, my_j + 1, rows, inner_k], dst_ref=field.at[t, their_j, rows, inner_k],
            send_sem=south_send.at[t, c], recv_sem=south_recv.at[t, c], **to("south", 1 - south))

    def east_copy(t, side):
        r, dst, other = (1, ni + 1, east - 1) if side == 0 else (ni, 0, east + 1)
        return pltpu.make_async_remote_copy(
            src_ref=field.at[t, pl.ds(1, nj), r, inner_k], dst_ref=field.at[t, pl.ds(1, nj), dst, inner_k],
            send_sem=east_send.at[t, side], recv_sem=east_recv.at[t, 1 - side], **to("east", other))

    def down_copy(t, c, side):
        other = down - 1 if side == 0 else down + 1
        return pltpu.make_async_remote_copy(
            src_ref=k_send.at[t, side, c], dst_ref=k_recv.at[t, 1 - side, c],
            send_sem=down_send.at[t, c, side], recv_sem=down_recv.at[t, c, 1 - side], **to("down", other))

    def detour_copy(t, c, side):
        return pltpu.make_async_remote_copy(
            src_ref=k_send.at[t, side, c], dst_ref=k_relay.at[t, c],
            send_sem=down_send.at[t, c, side], recv_sem=relay_recv.at[t, c],
            **to("down", own_base + route(t, c)))

    def hand_on_copy(t, c, side):
        return pltpu.make_async_remote_copy(
            src_ref=k_relay.at[t, c], dst_ref=k_recv.at[t, side, c],
            send_sem=relay_send.at[t, c], recv_sem=down_recv.at[t, c, side], **to("down", far_end))

    def send_down(t, c, near=None):
        def one(side):
            crosses = down == (half if side == 0 else half - 1)
            around = jnp.logical_and(crosses, own_base + route(t, c) != own_end)
            far = jnp.logical_and(crosses, jnp.logical_not(around))
            straight = jnp.logical_not(around)
            if near is not None:
                straight = far if not near else jnp.logical_not(crosses)

            if near is not False:
                @pl.when(around)
                def _():
                    detour_copy(t, c, side).start()

            @pl.when(straight)
            def _():
                down_copy(t, c, side).start()

        each(has_up, has_down, one)

    def hand_on(t, n):
        @pl.when(jnp.logical_and(is_relay, route(t, n) == mine))
        def _():
            pltpu.make_async_remote_copy(
                src_ref=k_relay.at[t, n], dst_ref=k_relay.at[t, n],
                send_sem=relay_send.at[t, n], recv_sem=relay_recv.at[t, n], **to("down", far_end)).wait_recv()
            hand_on_copy(t, n, own_side).start()

    def ends(t, c, w):
        r = row_of(c) + w + 1
        for j in range(nj):
            yield j + 1, r, pl.ds(w * nj + j, 1)

    def pack(t, c):
        def row(w, _):
            for j, r, at in ends(t, c, w):
                k_send[t, 0, c, at] = field[t, j, r, pl.ds(PAD, 1)]
                k_send[t, 1, c, at] = field[t, j, r, pl.ds(PAD + nk - 1, 1)]
            return 0

        lax.fori_loop(0, width, row, 0)

    def unpack(t, c):
        def row(w, _):
            for j, r, at in ends(t, c, w):
                field[t, j, r, pl.ds(PAD - 1, 1)] = k_recv[t, 0, c, at]
                field[t, j, r, pl.ds(PAD + nk, 1)] = k_recv[t, 1, c, at]
            return 0

        lax.fori_loop(0, width, row, 0)

    def advance(t, c, first, count, start=0, rows=width):
        def row(w, _):
            r = row_of(c) + start + w
            for b in range(nk // 8):
                at, here = pl.ds(PAD + 8 * b, 8), pl.ds(8 * b, 8)
                column = [field[t, first + p, r + 1, at] for p in range(count + 2)]
                for p in range(count):
                    j = first + p
                    mid, j_low, j_high = column[p + 1], column[p], column[p + 2]
                    i_low, i_high = field[t, j + 1, r, at], field[t, j + 1, r + 2, at]
                    k_low = field[t, j + 1, r + 1, pl.ds(PAD + 8 * b - 1, 8)]
                    k_high = field[t, j + 1, r + 1, pl.ds(PAD + 8 * b + 1, 8)]
                    spread = j_low + j_high + i_low + i_high + k_low + k_high - 6.0 * mid
                    value = (
                        mid - flow[0, j, r, here] * (j_high - j_low) - flow[1, j, r, here] * (i_high - i_low)
                        - flow[2, j, r, here] * (k_high - k_low) + SMOOTH * spread
                    )
                    if t == STEPS - 1:
                        out[j, r, here] = value
                    else:
                        field[t + 1, j + 1, r + 1, at] = value
            return 0

        lax.fori_loop(0, rows, row, 0, unroll=2)

    loads[0].wait()

    @pl.when(even)
    def _():
        pl.semaphore_wait(barrier, 3)
        pl.semaphore_signal(pair_sem.at[0], inc=1, **to("east", east + 1))

    @pl.when(odd)
    def _():
        pl.semaphore_wait(pair_sem.at[0], 1)

    south_copy(0, 0).start()
    for copy in loads[3:]:
        copy.start()
    loads[1].wait()
    loads[2].wait()

    def first_pack(c, _):
        pack(0, c)
        return 0

    lax.fori_loop(0, chunks, first_pack, 0)
    learn(1, 0, one(hub > 0, 2) + one(hub + 2 < n_east, 2) + one(near_up, 4) + one(near_down, 4)
          + one(at_seam, 4 * (half - 1)))
    each(has_west, has_east, lambda side: east_copy(0, side).start())

    def first_down(c, _):
        send_down(0, c, True)
        return 0

    lax.fori_loop(0, chunks, first_down, 0)

    outside_j = jnp.where(south == 0, 0, nj + 1)

    def clear(n, _):
        for t in range(STEPS):
            field[t, outside_j, n + 1, inner_k] = jnp.zeros((nk, ns), jnp.float32)
        return 0

    lax.fori_loop(0, ni, clear, 0)
    for edge, at in ((jnp.logical_not(has_west), 0), (jnp.logical_not(has_east), ni + 1)):
        @pl.when(edge)
        def _(at=at):
            for t in range(STEPS):
                for j in range(nj):
                    field[t, j + 1, at, inner_k] = jnp.zeros((nk, ns), jnp.float32)
    for edge, side in ((jnp.logical_not(has_up), 0), (jnp.logical_not(has_down), 1)):
        @pl.when(edge)
        def _(side=side):
            for t in range(STEPS):
                for c in range(chunks):
                    k_recv[t, side, c] = jnp.zeros(k_recv.shape[3:], jnp.float32)

    learn(2, 1, 4)

    def first_far(c, _):
        send_down(0, c, False)
        return 0

    lax.fori_loop(0, chunks, first_far, 0)
    for n in range(chunks):
        hand_on(0, jnp.int32(n))
    for c in range(1, lead):
        south_copy(0, c).start()
    for copy in loads[3:]:
        copy.wait()

    def pass_on(t, c):
        if t < STEPS - 1:
            @pl.when(c > 0)
            def _():
                hand_on(t + 1, c - 1)

        if t > 0:
            @pl.when(c == 0)
            def _():
                hand_on(t, c + chunks - 1)

    def arrive(t, c):
        south_copy(t, c).wait_recv()
        pass_on(t, c)

        @pl.when(c + lead < chunks - (1 if t == STEPS - 1 else 0))
        def _():
            south_copy(t, c + lead).start()

        if t == STEPS - 1:
            @pl.when(c + lead == chunks - 1)
            def _():
                for part in (0, 1):
                    south_copy(t, chunks - 1, part).start()

        if t < STEPS - 1:
            @pl.when(c + lead >= chunks)
            def _():
                south_copy(t + 1, c + lead - chunks).start()

    def surround(t, c):
        each(has_up, has_down, lambda side: down_copy(t, c, 1 - side).wait_recv())
        for side, cond in ((0, has_west), (1, has_east)):
            @pl.when(jnp.logical_and(cond, c == side))
            def _(side=side):
                east_copy(t, 1 - side).wait_recv()

        unpack(t, c)

    def sent(t, c):
        south_copy(t, c).wait_send()
        each(has_up, has_down, lambda side: down_copy(t, c, side).wait_send())

    for t in range(STEPS - 1):
        def chunk(c, _, t=t):
            arrive(t, c)
            surround(t, c)
            advance(t, c, 0, nj)
            pack(t + 1, c)
            send_down(t + 1, c)
            for side, cond in ((0, has_west), (1, has_east)):
                @pl.when(jnp.logical_and(cond, c == side))
                def _(side=side):
                    east_copy(t + 1, side).start()
            return 0

        lax.fori_loop(0, chunks, chunk, 0)

    t = STEPS - 1

    def last_chunk(c, _):
        early = c + lead < chunks

        @pl.when(early)
        def _():
            arrive(t, c)

        surround(t, c)
        advance(t, c, rest_j, nj - 1)

        @pl.when(c == chunks - 1)
        def _():
            def finish(n, _):
                for s in range(STEPS - 1):
                    sent(s, n)
                each(has_up, has_down, lambda side: down_copy(t, n, side).wait_send())
                return 0

            lax.fori_loop(0, chunks, finish, 0)
            for s in range(STEPS):
                each(has_west, has_east, lambda side: east_copy(s, side).wait_send())
                for n in range(chunks):
                    @pl.when(jnp.logical_and(is_relay, ROUTES[s][n] == mine))
                    def _(s=s, n=n):
                        hand_on_copy(s, n, 0).wait_send()

        @pl.when(jnp.logical_not(jnp.logical_or(early, c == chunks - 1)))
        def _():
            south_copy(t, c).wait_recv()

        @pl.when(c < chunks - 1)
        def _():
            advance(t, c, my_j, 1)

        @pl.when(c == chunks - 1)
        def _():
            for part in (0, 1):
                south_copy(t, chunks - 1, part).wait_recv()
                advance(t, c, my_j, 1, part * (width // 2), width // 2)

        return 0

    lax.fori_loop(0, chunks, last_chunk, 0)
    for c in range(chunks - 1):
        south_copy(t, c).wait_send()
    for part in (0, 1):
        south_copy(t, chunks - 1, part).wait_send()


def store_kernel(pieces, held, out, sem):
    nj, ni = held.shape[:2]
    step = nj * ni // pieces
    copies = [
        pltpu.make_async_copy(
            held.at[p * step // ni, pl.ds(p * step % ni, step)], out.at[p * step // ni, pl.ds(p * step % ni, step)], sem.at[p])
        for p in range(pieces)
    ]
    for copy in copies:
        copy.start()
    for copy in copies:
        copy.wait()


def solution(mesh, width=8, lead=2):
    sizes = tuple(mesh.shape[a] for a in ("south", "east", "down"))

    def per_device(density, flow_j, flow_i, flow_k):
        nj, ni, nk, ns = density.shape
        chunks = ni // width
        dma = pltpu.SemaphoreType.DMA
        held = pl.pallas_call(
            functools.partial(kernel, sizes, width, lead),
            out_shape=pltpu.VMEM(density.shape, density.dtype),
            in_specs=[pl.BlockSpec(memory_space=pl.ANY)] * 4,
            out_specs=pl.BlockSpec(memory_space=pltpu.VMEM),
            scratch_shapes=[
                pltpu.VMEM((STEPS, nj + 2, ni + 2, nk + 2 * PAD, ns), jnp.float32),
                pltpu.VMEM((3, nj, ni, nk, ns), jnp.float32),
                pltpu.VMEM((STEPS, 2, chunks, width * nj, ns), jnp.float32),
                pltpu.VMEM((STEPS, 2, chunks, width * nj, ns), jnp.float32),
                pltpu.VMEM((STEPS, chunks, width * nj, ns), jnp.float32),
                dma((6,)),
                dma((STEPS, chunks + 1)),
                dma((STEPS, chunks + 1)),
                dma((STEPS, 2)),
                dma((STEPS, 2)),
                dma((STEPS, chunks, 2)),
                dma((STEPS, chunks, 2)),
                dma((STEPS, chunks)),
                dma((STEPS, chunks)),
                pltpu.SemaphoreType.REGULAR((3,)),
            ],
            compiler_params=pltpu.CompilerParams(
                collective_id=0, has_side_effects=True, vmem_limit_bytes=48 * 1024 * 1024
            ),
            name="advect",
        )(density, flow_j, flow_i, flow_k)
        return pl.pallas_call(
            functools.partial(store_kernel, nj),
            out_shape=jax.ShapeDtypeStruct(density.shape, density.dtype),
            in_specs=[pl.BlockSpec(memory_space=pltpu.VMEM)],
            out_specs=pl.BlockSpec(memory_space=pl.ANY),
            scratch_shapes=[dma((nj,))],
            compiler_params=pltpu.CompilerParams(vmem_limit_bytes=8 * 1024 * 1024),
            name="store",
        )(held)

    spec = P(("ens", "south"), "east", "down", None)
    return jax.shard_map(per_device, mesh=mesh, in_specs=(spec,) * 4, out_specs=spec, check_vma=False)
```

```python
import functools

import jax
import jax.numpy as jnp
from jax import lax
from jax.experimental import pallas as pl
from jax.experimental.pallas import tpu as pltpu
from jax.sharding import PartitionSpec as P

STEPS = 3
SMOOTH = 0.05
PAD = 8
ROUTES = ((0, 1, 2, 3), (1, 2, 3, 1), (2, 1, 3, 2))


def kernel(
    sizes, width, lead, den, fj, fi, fk, out, field, flow, k_send, k_recv, k_relay,
    load_sem, south_send, south_recv, east_send, east_recv, down_send, down_recv, relay_send, relay_recv, pair_sem,
):
    _, n_east, n_down = sizes
    nj, ni, nk, ns = den.shape
    chunks = ni // width
    half = n_down // 2
    assert chunks == len(ROUTES[0]) == half
    south, east, down = (lax.axis_index(a) for a in ("south", "east", "down"))
    has_west, has_east = east > 0, east < n_east - 1
    has_up, has_down = down > 0, down < n_down - 1
    inner_k = pl.ds(PAD, nk)
    my_j = jnp.where(south == 0, nj - 1, 0)
    their_j = jnp.where(south == 0, 0, nj + 1)
    rest_j = jnp.where(south == 0, 0, 1)

    def to(axis, index):
        return dict(device_id={axis: index}, device_id_type=pl.DeviceIdType.MESH)

    def each(cond_low, cond_high, fn):
        for side, cond in ((0, cond_low), (1, cond_high)):
            @pl.when(cond)
            def _(side=side):
                fn(side)

    def row_of(c):
        return width * jnp.where(c == 0, 0, jnp.where(c == 1, chunks - 1, c - 1))

    lower = down < half
    at_seam = jnp.logical_or(down == half - 1, down == half)
    mine = lax.rem(down, half)
    own_end = jnp.where(lower, half - 1, half)
    far_end = jnp.where(lower, half, half - 1)
    far_base = jnp.where(lower, half, 0)
    own_base = jnp.where(lower, 0, half)
    own_side = jnp.where(lower, 0, 1)
    is_relay = jnp.logical_not(at_seam)
    def route(t, c):
        n = ROUTES[t][0]
        for x in range(1, chunks):
            n = jnp.where(c == x, ROUTES[t][x], n)
        return n


    def plane_load(n, first, count):
        return pltpu.make_async_copy(
            den.at[my_j, pl.ds(first, count)], field.at[0, my_j + 1, pl.ds(first + 1, count), inner_k], load_sem.at[n])

    loads = [
        plane_load(0, 0, width),
        plane_load(1, width, ni - width),
        pltpu.make_async_copy(
            den.at[pl.ds(rest_j, nj - 1)], field.at[0, pl.ds(rest_j + 1, nj - 1), pl.ds(1, ni), inner_k], load_sem.at[2]),
    ]
    for x, src in enumerate((fj, fi, fk)):
        loads.append(pltpu.make_async_copy(src, flow.at[x], load_sem.at[x + 3]))

    even = lax.rem(east, 2) == 0
    odd = jnp.logical_not(even)
    base = east - lax.rem(east, 2)
    hub = base + 1
    barrier = pltpu.get_barrier_semaphore()

    def hello(cond, index, **others):
        @pl.when(cond)
        def _():
            pl.semaphore_signal(
                barrier, inc=1, device_id={"east": index, **others}, device_id_type=pl.DeviceIdType.MESH)

    near_up = jnp.logical_and(has_up, down != half)
    near_down = jnp.logical_and(has_down, down != half - 1)
    loads[0].start()
    hello(down >= 0, hub, south=1 - south)
    hello(even, hub)
    hello(jnp.logical_and(even, has_west), east - 2, south=0)
    hello(jnp.logical_and(odd, has_east), east + 1, south=0)
    hello(near_up, base, south=0, down=down - 1)
    hello(near_down, base, south=0, down=down + 1)
    hello(is_relay, base, south=0, down=own_end)
    for m in range(half):
        hello(at_seam, base, south=1, down=far_base + m)

    def one(cond, n):
        return jnp.where(cond, n, 0)

    def learn(n, who, count):
        taker = jnp.logical_and(even, south == who)

        @pl.when(taker)
        def _():
            pl.semaphore_wait(barrier, count)
            for s, e in ((who, hub), (1 - who, hub), (1 - who, base)):
                pl.semaphore_signal(
                    pair_sem.at[n], inc=1, device_id={"south": s, "east": e}, device_id_type=pl.DeviceIdType.MESH)

        @pl.when(jnp.logical_not(taker))
        def _():
            pl.semaphore_wait(pair_sem.at[n], 1)

    for copy in loads[1:3]:
        copy.start()

    def south_copy(t, c, part=None):
        if part is None:
            rows = pl.ds(row_of(c) + 1, width)
        else:
            rows = pl.ds(row_of(c) + 1 + part * (width // 2), width // 2)
            c = chunks - 1 + part
        return pltpu.make_async_remote_copy(
            src_ref=field.at[t, my_j + 1, rows, inner_k], dst_ref=field.at[t, their_j, rows, inner_k],
            send_sem=south_send.at[t, c], recv_sem=south_recv.at[t, c], **to("south", 1 - south))

    def east_copy(t, side):
        r, dst, other = (1, ni + 1, east - 1) if side == 0 else (ni, 0, east + 1)
        return pltpu.make_async_remote_copy(
            src_ref=field.at[t, pl.ds(1, nj), r, inner_k], dst_ref=field.at[t, pl.ds(1, nj), dst, inner_k],
            send_sem=east_send.at[t, side], recv_sem=east_recv.at[t, 1 - side], **to("east", other))

    def down_copy(t, c, side):
        other = down - 1 if side == 0 else down + 1
        return pltpu.make_async_remote_copy(
            src_ref=k_send.at[t, side, c], dst_ref=k_recv.at[t, 1 - side, c],
            send_sem=down_send.at[t, c, side], recv_sem=down_recv.at[t, c, 1 - side], **to("down", other))

    def detour_copy(t, c, side):
        return pltpu.make_async_remote_copy(
            src_ref=k_send.at[t, side, c], dst_ref=k_relay.at[t, c],
            send_sem=down_send.at[t, c, side], recv_sem=relay_recv.at[t, c],
            **to("down", own_base + route(t, c)))

    def hand_on_copy(t, c, side):
        return pltpu.make_async_remote_copy(
            src_ref=k_relay.at[t, c], dst_ref=k_recv.at[t, side, c],
            send_sem=relay_send.at[t, c], recv_sem=down_recv.at[t, c, side], **to("down", far_end))

    def send_down(t, c, near=None):
        def one(side):
            crosses = down == (half if side == 0 else half - 1)
            around = jnp.logical_and(crosses, own_base + route(t, c) != own_end)
            far = jnp.logical_and(crosses, jnp.logical_not(around))
            straight = jnp.logical_not(around)
            if near is not None:
                straight = far if not near else jnp.logical_not(crosses)

            if near is not False:
                @pl.when(around)
                def _():
                    detour_copy(t, c, side).start()

            @pl.when(straight)
            def _():
                down_copy(t, c, side).start()

        each(has_up, has_down, one)

    def hand_on(t, n):
        @pl.when(jnp.logical_and(is_relay, route(t, n) == mine))
        def _():
            pltpu.make_async_remote_copy(
                src_ref=k_relay.at[t, n], dst_ref=k_relay.at[t, n],
                send_sem=relay_send.at[t, n], recv_sem=relay_recv.at[t, n], **to("down", far_end)).wait_recv()
            hand_on_copy(t, n, own_side).start()

    def ends(t, c, w):
        r = row_of(c) + w + 1
        for j in range(nj):
            yield j + 1, r, pl.ds(w * nj + j, 1)

    def pack(t, c):
        def row(w, _):
            for j, r, at in ends(t, c, w):
                k_send[t, 0, c, at] = field[t, j, r, pl.ds(PAD, 1)]
                k_send[t, 1, c, at] = field[t, j, r, pl.ds(PAD + nk - 1, 1)]
            return 0

        lax.fori_loop(0, width, row, 0)

    def unpack(t, c):
        def row(w, _):
            for j, r, at in ends(t, c, w):
                field[t, j, r, pl.ds(PAD - 1, 1)] = k_recv[t, 0, c, at]
                field[t, j, r, pl.ds(PAD + nk, 1)] = k_recv[t, 1, c, at]
            return 0

        lax.fori_loop(0, width, row, 0)

    def advance(t, c, first, count, start=0, rows=width):
        def row(w, _):
            r = row_of(c) + start + w
            for b in range(nk // 8):
                at, here = pl.ds(PAD + 8 * b, 8), pl.ds(8 * b, 8)
                column = [field[t, first + p, r + 1, at] for p in range(count + 2)]
                for p in range(count):
                    j = first + p
                    mid, j_low, j_high = column[p + 1], column[p], column[p + 2]
                    i_low, i_high = field[t, j + 1, r, at], field[t, j + 1, r + 2, at]
                    k_low = field[t, j + 1, r + 1, pl.ds(PAD + 8 * b - 1, 8)]
                    k_high = field[t, j + 1, r + 1, pl.ds(PAD + 8 * b + 1, 8)]
                    spread = j_low + j_high + i_low + i_high + k_low + k_high - 6.0 * mid
                    value = (
                        mid - flow[0, j, r, here] * (j_high - j_low) - flow[1, j, r, here] * (i_high - i_low)
                        - flow[2, j, r, here] * (k_high - k_low) + SMOOTH * spread
                    )
                    if t == STEPS - 1:
                        out[j, r, here] = value
                    else:
                        field[t + 1, j + 1, r + 1, at] = value
            return 0

        lax.fori_loop(0, rows, row, 0, unroll=2)

    loads[0].wait()

    @pl.when(odd)
    def _():
        pl.semaphore_wait(barrier, 3)
        pl.semaphore_signal(pair_sem.at[0], inc=1, **to("east", east - 1))

    @pl.when(even)
    def _():
        pl.semaphore_wait(pair_sem.at[0], 1)

    south_copy(0, 0).start()
    for copy in loads[3:]:
        copy.start()
    loads[1].wait()
    loads[2].wait()

    def first_pack(c, _):
        pack(0, c)
        return 0

    lax.fori_loop(0, chunks, first_pack, 0)
    learn(1, 0, one(base > 0, 2) + one(base + 2 < n_east, 2) + one(near_up, 4) + one(near_down, 4)
          + one(at_seam, 4 * (half - 1)))
    each(has_west, has_east, lambda side: east_copy(0, side).start())

    def first_down(c, _):
        send_down(0, c, True)
        return 0

    lax.fori_loop(0, chunks, first_down, 0)

    outside_j = jnp.where(south == 0, 0, nj + 1)

    def clear(n, _):
        for t in range(STEPS):
            field[t, outside_j, n + 1, inner_k] = jnp.zeros((nk, ns), jnp.float32)
        return 0

    lax.fori_loop(0, ni, clear, 0)
    for edge, at in ((jnp.logical_not(has_west), 0), (jnp.logical_not(has_east), ni + 1)):
        @pl.when(edge)
        def _(at=at):
            for t in range(STEPS):
                for j in range(nj):
                    field[t, j + 1, at, inner_k] = jnp.zeros((nk, ns), jnp.float32)
    for edge, side in ((jnp.logical_not(has_up), 0), (jnp.logical_not(has_down), 1)):
        @pl.when(edge)
        def _(side=side):
            for t in range(STEPS):
                for c in range(chunks):
                    k_recv[t, side, c] = jnp.zeros(k_recv.shape[3:], jnp.float32)

    learn(2, 1, 4)

    def first_far(c, _):
        send_down(0, c, False)
        return 0

    lax.fori_loop(0, chunks, first_far, 0)
    for n in range(chunks):
        hand_on(0, jnp.int32(n))
    for c in range(1, lead):
        south_copy(0, c).start()
    for copy in loads[3:]:
        copy.wait()

    def pass_on(t, c):
        if t < STEPS - 1:
            @pl.when(c > 0)
            def _():
                hand_on(t + 1, c - 1)

        if t > 0:
            @pl.when(c == 0)
            def _():
                hand_on(t, c + chunks - 1)

    def arrive(t, c):
        south_copy(t, c).wait_recv()
        pass_on(t, c)

        @pl.when(c + lead < chunks - (1 if t == STEPS - 1 else 0))
        def _():
            south_copy(t, c + lead).start()

        if t == STEPS - 1:
            @pl.when(c + lead == chunks - 1)
            def _():
                for part in (0, 1):
                    south_copy(t, chunks - 1, part).start()

        if t < STEPS - 1:
            @pl.when(c + lead >= chunks)
            def _():
                south_copy(t + 1, c + lead - chunks).start()

    def surround(t, c):
        each(has_up, has_down, lambda side: down_copy(t, c, 1 - side).wait_recv())
        for side, cond in ((0, has_west), (1, has_east)):
            @pl.when(jnp.logical_and(cond, c == side))
            def _(side=side):
                east_copy(t, 1 - side).wait_recv()

        unpack(t, c)

    def sent(t, c):
        south_copy(t, c).wait_send()
        each(has_up, has_down, lambda side: down_copy(t, c, side).wait_send())

    for t in range(STEPS - 1):
        def chunk(c, _, t=t):
            arrive(t, c)
            surround(t, c)
            advance(t, c, 0, nj)
            pack(t + 1, c)
            send_down(t + 1, c)
            for side, cond in ((0, has_west), (1, has_east)):
                @pl.when(jnp.logical_and(cond, c == side))
                def _(side=side):
                    east_copy(t + 1, side).start()
            return 0

        lax.fori_loop(0, chunks, chunk, 0)

    t = STEPS - 1

    def last_chunk(c, _):
        early = c + lead < chunks

        @pl.when(early)
        def _():
            arrive(t, c)

        surround(t, c)
        advance(t, c, rest_j, nj - 1)

        @pl.when(c == chunks - 1)
        def _():
            def finish(n, _):
                for s in range(STEPS - 1):
                    sent(s, n)
                each(has_up, has_down, lambda side: down_copy(t, n, side).wait_send())
                return 0

            lax.fori_loop(0, chunks, finish, 0)
            for s in range(STEPS):
                each(has_west, has_east, lambda side: east_copy(s, side).wait_send())
                for n in range(chunks):
                    @pl.when(jnp.logical_and(is_relay, ROUTES[s][n] == mine))
                    def _(s=s, n=n):
                        hand_on_copy(s, n, 0).wait_send()

        @pl.when(jnp.logical_not(jnp.logical_or(early, c == chunks - 1)))
        def _():
            south_copy(t, c).wait_recv()

        @pl.when(c < chunks - 1)
        def _():
            advance(t, c, my_j, 1)

        @pl.when(c == chunks - 1)
        def _():
            for part in (0, 1):
                south_copy(t, chunks - 1, part).wait_recv()
                advance(t, c, my_j, 1, part * (width // 2), width // 2)

        return 0

    lax.fori_loop(0, chunks, last_chunk, 0)
    for c in range(chunks - 1):
        south_copy(t, c).wait_send()
    for part in (0, 1):
        south_copy(t, chunks - 1, part).wait_send()


def store_kernel(pieces, held, out, sem):
    nj, ni = held.shape[:2]
    step = nj * ni // pieces
    copies = [
        pltpu.make_async_copy(
            held.at[p * step // ni, pl.ds(p * step % ni, step)], out.at[p * step // ni, pl.ds(p * step % ni, step)], sem.at[p])
        for p in range(pieces)
    ]
    for copy in copies:
        copy.start()
    for copy in copies:
        copy.wait()


def solution(mesh, width=8, lead=2):
    sizes = tuple(mesh.shape[a] for a in ("south", "east", "down"))

    def per_device(density, flow_j, flow_i, flow_k):
        nj, ni, nk, ns = density.shape
        chunks = ni // width
        dma = pltpu.SemaphoreType.DMA
        held = pl.pallas_call(
            functools.partial(kernel, sizes, width, lead),
            out_shape=pltpu.VMEM(density.shape, density.dtype),
            in_specs=[pl.BlockSpec(memory_space=pl.ANY)] * 4,
            out_specs=pl.BlockSpec(memory_space=pltpu.VMEM),
            scratch_shapes=[
                pltpu.VMEM((STEPS, nj + 2, ni + 2, nk + 2 * PAD, ns), jnp.float32),
                pltpu.VMEM((3, nj, ni, nk, ns), jnp.float32),
                pltpu.VMEM((STEPS, 2, chunks, width * nj, ns), jnp.float32),
                pltpu.VMEM((STEPS, 2, chunks, width * nj, ns), jnp.float32),
                pltpu.VMEM((STEPS, chunks, width * nj, ns), jnp.float32),
                dma((6,)),
                dma((STEPS, chunks + 1)),
                dma((STEPS, chunks + 1)),
                dma((STEPS, 2)),
                dma((STEPS, 2)),
                dma((STEPS, chunks, 2)),
                dma((STEPS, chunks, 2)),
                dma((STEPS, chunks)),
                dma((STEPS, chunks)),
                pltpu.SemaphoreType.REGULAR((3,)),
            ],
            compiler_params=pltpu.CompilerParams(
                collective_id=0, has_side_effects=True, vmem_limit_bytes=48 * 1024 * 1024
            ),
            name="advect",
        )(density, flow_j, flow_i, flow_k)
        return pl.pallas_call(
            functools.partial(store_kernel, nj),
            out_shape=jax.ShapeDtypeStruct(density.shape, density.dtype),
            in_specs=[pl.BlockSpec(memory_space=pltpu.VMEM)],
            out_specs=pl.BlockSpec(memory_space=pl.ANY),
            scratch_shapes=[dma((nj,))],
            compiler_params=pltpu.CompilerParams(vmem_limit_bytes=8 * 1024 * 1024),
            name="store",
        )(held)

    spec = P(("ens", "south"), "east", "down", None)
    return jax.shard_map(per_device, mesh=mesh, in_specs=(spec,) * 4, out_specs=spec, check_vma=False)
```

```python
import functools

import jax
import jax.numpy as jnp
from jax import lax
from jax.experimental import pallas as pl
from jax.experimental.pallas import tpu as pltpu
from jax.sharding import PartitionSpec as P

STEPS = 3
SMOOTH = 0.05
PAD = 8
ROUTES = ((0, 1, 2, 3), (1, 3, 2, 0), (2, 1, 3, 3))


def kernel(
    sizes, width, lead, den, fj, fi, fk, out, field, flow, k_send, k_recv, k_relay,
    load_sem, south_send, south_recv, east_send, east_recv, down_send, down_recv, relay_send, relay_recv, pair_sem,
):
    _, n_east, n_down = sizes
    nj, ni, nk, ns = den.shape
    chunks = ni // width
    half = n_down // 2
    assert chunks == len(ROUTES[0]) == half
    south, east, down = (lax.axis_index(a) for a in ("south", "east", "down"))
    has_west, has_east = east > 0, east < n_east - 1
    has_up, has_down = down > 0, down < n_down - 1
    inner_k = pl.ds(PAD, nk)
    my_j = jnp.where(south == 0, nj - 1, 0)
    their_j = jnp.where(south == 0, 0, nj + 1)
    rest_j = jnp.where(south == 0, 0, 1)

    def to(axis, index):
        return dict(device_id={axis: index}, device_id_type=pl.DeviceIdType.MESH)

    def each(cond_low, cond_high, fn):
        for side, cond in ((0, cond_low), (1, cond_high)):
            @pl.when(cond)
            def _(side=side):
                fn(side)

    def row_of(c):
        return width * jnp.where(c == 0, 0, jnp.where(c == 1, chunks - 1, c - 1))

    lower = down < half
    at_seam = jnp.logical_or(down == half - 1, down == half)
    mine = lax.rem(down, half)
    own_end = jnp.where(lower, half - 1, half)
    far_end = jnp.where(lower, half, half - 1)
    far_base = jnp.where(lower, half, 0)
    own_base = jnp.where(lower, 0, half)
    own_side = jnp.where(lower, 0, 1)
    is_relay = jnp.logical_not(at_seam)
    def route(t, c):
        n = ROUTES[t][0]
        for x in range(1, chunks):
            n = jnp.where(c == x, ROUTES[t][x], n)
        return n


    def plane_load(n, first, count):
        return pltpu.make_async_copy(
            den.at[my_j, pl.ds(first, count)], field.at[0, my_j + 1, pl.ds(first + 1, count), inner_k], load_sem.at[n])

    loads = [
        plane_load(0, 0, width),
        plane_load(1, width, ni - width),
        pltpu.make_async_copy(
            den.at[pl.ds(rest_j, nj - 1)], field.at[0, pl.ds(rest_j + 1, nj - 1), pl.ds(1, ni), inner_k], load_sem.at[2]),
    ]
    for x, src in enumerate((fj, fi, fk)):
        loads.append(pltpu.make_async_copy(src, flow.at[x], load_sem.at[x + 3]))

    even = lax.rem(east, 2) == 0
    odd = jnp.logical_not(even)
    base = east - lax.rem(east, 2)
    hub = base + 1
    barrier = pltpu.get_barrier_semaphore()

    def hello(cond, index, **others):
        @pl.when(cond)
        def _():
            pl.semaphore_signal(
                barrier, inc=1, device_id={"east": index, **others}, device_id_type=pl.DeviceIdType.MESH)

    near_up = jnp.logical_and(has_up, down != half)
    near_down = jnp.logical_and(has_down, down != half - 1)
    loads[0].start()
    hello(down >= 0, hub, south=1 - south)
    hello(even, hub)
    hello(jnp.logical_and(even, has_west), east - 2, south=0)
    hello(jnp.logical_and(odd, has_east), east + 1, south=0)
    hello(near_up, base, south=0, down=down - 1)
    hello(near_down, base, south=0, down=down + 1)
    hello(is_relay, base, south=0, down=own_end)
    for m in range(half):
        hello(at_seam, base, south=1, down=far_base + m)

    def one(cond, n):
        return jnp.where(cond, n, 0)

    def learn(n, who, count):
        taker = jnp.logical_and(even, south == who)

        @pl.when(taker)
        def _():
            pl.semaphore_wait(barrier, count)
            for s, e in ((who, hub), (1 - who, hub), (1 - who, base)):
                pl.semaphore_signal(
                    pair_sem.at[n], inc=1, device_id={"south": s, "east": e}, device_id_type=pl.DeviceIdType.MESH)

        @pl.when(jnp.logical_not(taker))
        def _():
            pl.semaphore_wait(pair_sem.at[n], 1)

    for copy in loads[1:3]:
        copy.start()

    def south_copy(t, c, part=None):
        if part is None:
            rows = pl.ds(row_of(c) + 1, width)
        else:
            rows = pl.ds(row_of(c) + 1 + part * (width // 2), width // 2)
            c = chunks - 1 + part
        return pltpu.make_async_remote_copy(
            src_ref=field.at[t, my_j + 1, rows, inner_k], dst_ref=field.at[t, their_j, rows, inner_k],
            send_sem=south_send.at[t, c], recv_sem=south_recv.at[t, c], **to("south", 1 - south))

    def east_copy(t, side):
        r, dst, other = (1, ni + 1, east - 1) if side == 0 else (ni, 0, east + 1)
        return pltpu.make_async_remote_copy(
            src_ref=field.at[t, pl.ds(1, nj), r, inner_k], dst_ref=field.at[t, pl.ds(1, nj), dst, inner_k],
            send_sem=east_send.at[t, side], recv_sem=east_recv.at[t, 1 - side], **to("east", other))

    def down_copy(t, c, side):
        other = down - 1 if side == 0 else down + 1
        return pltpu.make_async_remote_copy(
            src_ref=k_send.at[t, side, c], dst_ref=k_recv.at[t, 1 - side, c],
            send_sem=down_send.at[t, c, side], recv_sem=down_recv.at[t, c, 1 - side], **to("down", other))

    def detour_copy(t, c, side):
        return pltpu.make_async_remote_copy(
            src_ref=k_send.at[t, side, c], dst_ref=k_relay.at[t, c],
            send_sem=down_send.at[t, c, side], recv_sem=relay_recv.at[t, c],
            **to("down", own_base + route(t, c)))

    def hand_on_copy(t, c, side):
        return pltpu.make_async_remote_copy(
            src_ref=k_relay.at[t, c], dst_ref=k_recv.at[t, side, c],
            send_sem=relay_send.at[t, c], recv_sem=down_recv.at[t, c, side], **to("down", far_end))

    def send_down(t, c, near=None):
        def one(side):
            crosses = down == (half if side == 0 else half - 1)
            around = jnp.logical_and(crosses, own_base + route(t, c) != own_end)
            far = jnp.logical_and(crosses, jnp.logical_not(around))
            straight = jnp.logical_not(around)
            if near is not None:
                straight = far if not near else jnp.logical_not(crosses)

            if near is not False:
                @pl.when(around)
                def _():
                    detour_copy(t, c, side).start()

            @pl.when(straight)
            def _():
                down_copy(t, c, side).start()

        each(has_up, has_down, one)

    def hand_on(t, n):
        @pl.when(jnp.logical_and(is_relay, route(t, n) == mine))
        def _():
            pltpu.make_async_remote_copy(
                src_ref=k_relay.at[t, n], dst_ref=k_relay.at[t, n],
                send_sem=relay_send.at[t, n], recv_sem=relay_recv.at[t, n], **to("down", far_end)).wait_recv()
            hand_on_copy(t, n, own_side).start()

    def ends(t, c, w):
        r = row_of(c) + w + 1
        for j in range(nj):
            yield j + 1, r, pl.ds(w * nj + j, 1)

    def pack(t, c):
        def row(w, _):
            for j, r, at in ends(t, c, w):
                k_send[t, 0, c, at] = field[t, j, r, pl.ds(PAD, 1)]
                k_send[t, 1, c, at] = field[t, j, r, pl.ds(PAD + nk - 1, 1)]
            return 0

        lax.fori_loop(0, width, row, 0)

    def unpack(t, c):
        def row(w, _):
            for j, r, at in ends(t, c, w):
                field[t, j, r, pl.ds(PAD - 1, 1)] = k_recv[t, 0, c, at]
                field[t, j, r, pl.ds(PAD + nk, 1)] = k_recv[t, 1, c, at]
            return 0

        lax.fori_loop(0, width, row, 0)

    def advance(t, c, first, count, start=0, rows=width):
        def row(w, _):
            r = row_of(c) + start + w
            for b in range(nk // 8):
                at, here = pl.ds(PAD + 8 * b, 8), pl.ds(8 * b, 8)
                column = [field[t, first + p, r + 1, at] for p in range(count + 2)]
                for p in range(count):
                    j = first + p
                    mid, j_low, j_high = column[p + 1], column[p], column[p + 2]
                    i_low, i_high = field[t, j + 1, r, at], field[t, j + 1, r + 2, at]
                    k_low = field[t, j + 1, r + 1, pl.ds(PAD + 8 * b - 1, 8)]
                    k_high = field[t, j + 1, r + 1, pl.ds(PAD + 8 * b + 1, 8)]
                    spread = j_low + j_high + i_low + i_high + k_low + k_high - 6.0 * mid
                    value = (
                        mid - flow[0, j, r, here] * (j_high - j_low) - flow[1, j, r, here] * (i_high - i_low)
                        - flow[2, j, r, here] * (k_high - k_low) + SMOOTH * spread
                    )
                    if t == STEPS - 1:
                        out[j, r, here] = value
                    else:
                        field[t + 1, j + 1, r + 1, at] = value
            return 0

        lax.fori_loop(0, rows, row, 0, unroll=2)

    loads[0].wait()

    @pl.when(odd)
    def _():
        pl.semaphore_wait(barrier, 3)
        pl.semaphore_signal(pair_sem.at[0], inc=1, **to("east", east - 1))

    @pl.when(even)
    def _():
        pl.semaphore_wait(pair_sem.at[0], 1)

    south_copy(0, 0).start()
    for copy in loads[3:]:
        copy.start()
    loads[1].wait()
    loads[2].wait()

    def first_pack(c, _):
        pack(0, c)
        return 0

    lax.fori_loop(0, chunks, first_pack, 0)
    learn(1, 0, one(base > 0, 2) + one(base + 2 < n_east, 2) + one(near_up, 4) + one(near_down, 4)
          + one(at_seam, 4 * (half - 1)))
    each(has_west, has_east, lambda side: east_copy(0, side).start())

    def first_down(c, _):
        send_down(0, c, True)
        return 0

    lax.fori_loop(0, chunks, first_down, 0)

    outside_j = jnp.where(south == 0, 0, nj + 1)

    def clear(n, _):
        for t in range(STEPS):
            field[t, outside_j, n + 1, inner_k] = jnp.zeros((nk, ns), jnp.float32)
        return 0

    lax.fori_loop(0, ni, clear, 0)
    for edge, at in ((jnp.logical_not(has_west), 0), (jnp.logical_not(has_east), ni + 1)):
        @pl.when(edge)
        def _(at=at):
            for t in range(STEPS):
                for j in range(nj):
                    field[t, j + 1, at, inner_k] = jnp.zeros((nk, ns), jnp.float32)
    for edge, side in ((jnp.logical_not(has_up), 0), (jnp.logical_not(has_down), 1)):
        @pl.when(edge)
        def _(side=side):
            for t in range(STEPS):
                for c in range(chunks):
                    k_recv[t, side, c] = jnp.zeros(k_recv.shape[3:], jnp.float32)

    learn(2, 1, 4)

    def first_far(c, _):
        send_down(0, c, False)
        return 0

    lax.fori_loop(0, chunks, first_far, 0)
    for n in range(chunks):
        hand_on(0, jnp.int32(n))
    for c in range(1, lead):
        south_copy(0, c).start()
    for copy in loads[3:]:
        copy.wait()

    def pass_on(t, c):
        if t < STEPS - 1:
            @pl.when(c > 0)
            def _():
                hand_on(t + 1, c - 1)

        if t > 0:
            @pl.when(c == 0)
            def _():
                hand_on(t, c + chunks - 1)

    def arrive(t, c):
        south_copy(t, c).wait_recv()
        pass_on(t, c)

        @pl.when(c + lead < chunks - (1 if t == STEPS - 1 else 0))
        def _():
            south_copy(t, c + lead).start()

        if t == STEPS - 1:
            @pl.when(c + lead == chunks - 1)
            def _():
                for part in (0, 1):
                    south_copy(t, chunks - 1, part).start()

        if t < STEPS - 1:
            @pl.when(c + lead >= chunks)
            def _():
                south_copy(t + 1, c + lead - chunks).start()

    def surround(t, c):
        each(has_up, has_down, lambda side: down_copy(t, c, 1 - side).wait_recv())
        for side, cond in ((0, has_west), (1, has_east)):
            @pl.when(jnp.logical_and(cond, c == side))
            def _(side=side):
                east_copy(t, 1 - side).wait_recv()

        unpack(t, c)

    def sent(t, c):
        south_copy(t, c).wait_send()
        each(has_up, has_down, lambda side: down_copy(t, c, side).wait_send())

    for t in range(STEPS - 1):
        def chunk(c, _, t=t):
            arrive(t, c)
            surround(t, c)
            advance(t, c, 0, nj)
            pack(t + 1, c)
            send_down(t + 1, c)
            for side, cond in ((0, has_west), (1, has_east)):
                @pl.when(jnp.logical_and(cond, c == side))
                def _(side=side):
                    east_copy(t + 1, side).start()
            return 0

        lax.fori_loop(0, chunks, chunk, 0)

    t = STEPS - 1

    def last_chunk(c, _):
        early = c + lead < chunks

        @pl.when(early)
        def _():
            arrive(t, c)

        surround(t, c)
        advance(t, c, rest_j, nj - 1)

        @pl.when(c == chunks - 1)
        def _():
            def finish(n, _):
                for s in range(STEPS - 1):
                    sent(s, n)
                each(has_up, has_down, lambda side: down_copy(t, n, side).wait_send())
                return 0

            lax.fori_loop(0, chunks, finish, 0)
            for s in range(STEPS):
                each(has_west, has_east, lambda side: east_copy(s, side).wait_send())
                for n in range(chunks):
                    @pl.when(jnp.logical_and(is_relay, ROUTES[s][n] == mine))
                    def _(s=s, n=n):
                        hand_on_copy(s, n, 0).wait_send()

        @pl.when(jnp.logical_not(jnp.logical_or(early, c == chunks - 1)))
        def _():
            south_copy(t, c).wait_recv()

        @pl.when(c < chunks - 1)
        def _():
            advance(t, c, my_j, 1)

        @pl.when(c == chunks - 1)
        def _():
            for part in (0, 1):
                south_copy(t, chunks - 1, part).wait_recv()
                advance(t, c, my_j, 1, part * (width // 2), width // 2)

        return 0

    lax.fori_loop(0, chunks, last_chunk, 0)
    for c in range(chunks - 1):
        south_copy(t, c).wait_send()
    for part in (0, 1):
        south_copy(t, chunks - 1, part).wait_send()


def store_kernel(pieces, held, out, sem):
    nj, ni = held.shape[:2]
    step = nj * ni // pieces
    copies = [
        pltpu.make_async_copy(
            held.at[p * step // ni, pl.ds(p * step % ni, step)], out.at[p * step // ni, pl.ds(p * step % ni, step)], sem.at[p])
        for p in range(pieces)
    ]
    for copy in copies:
        copy.start()
    for copy in copies:
        copy.wait()


def solution(mesh, width=8, lead=2):
    sizes = tuple(mesh.shape[a] for a in ("south", "east", "down"))

    def per_device(density, flow_j, flow_i, flow_k):
        nj, ni, nk, ns = density.shape
        chunks = ni // width
        dma = pltpu.SemaphoreType.DMA
        held = pl.pallas_call(
            functools.partial(kernel, sizes, width, lead),
            out_shape=pltpu.VMEM(density.shape, density.dtype),
            in_specs=[pl.BlockSpec(memory_space=pl.ANY)] * 4,
            out_specs=pl.BlockSpec(memory_space=pltpu.VMEM),
            scratch_shapes=[
                pltpu.VMEM((STEPS, nj + 2, ni + 2, nk + 2 * PAD, ns), jnp.float32),
                pltpu.VMEM((3, nj, ni, nk, ns), jnp.float32),
                pltpu.VMEM((STEPS, 2, chunks, width * nj, ns), jnp.float32),
                pltpu.VMEM((STEPS, 2, chunks, width * nj, ns), jnp.float32),
                pltpu.VMEM((STEPS, chunks, width * nj, ns), jnp.float32),
                dma((6,)),
                dma((STEPS, chunks + 1)),
                dma((STEPS, chunks + 1)),
                dma((STEPS, 2)),
                dma((STEPS, 2)),
                dma((STEPS, chunks, 2)),
                dma((STEPS, chunks, 2)),
                dma((STEPS, chunks)),
                dma((STEPS, chunks)),
                pltpu.SemaphoreType.REGULAR((3,)),
            ],
            compiler_params=pltpu.CompilerParams(
                collective_id=0, has_side_effects=True, vmem_limit_bytes=48 * 1024 * 1024
            ),
            name="advect",
        )(density, flow_j, flow_i, flow_k)
        return pl.pallas_call(
            functools.partial(store_kernel, nj),
            out_shape=jax.ShapeDtypeStruct(density.shape, density.dtype),
            in_specs=[pl.BlockSpec(memory_space=pltpu.VMEM)],
            out_specs=pl.BlockSpec(memory_space=pl.ANY),
            scratch_shapes=[dma((nj,))],
            compiler_params=pltpu.CompilerParams(vmem_limit_bytes=8 * 1024 * 1024),
            name="store",
        )(held)

    spec = P(("ens", "south"), "east", "down", None)
    return jax.shard_map(per_device, mesh=mesh, in_specs=(spec,) * 4, out_specs=spec, check_vma=False)
```

```python
import functools

import jax
import jax.numpy as jnp
from jax import lax
from jax.experimental import pallas as pl
from jax.experimental.pallas import tpu as pltpu
from jax.sharding import PartitionSpec as P

STEPS = 3
SMOOTH = 0.05
PARTS = 4
PAD = 8
ROUTES = ((0, 1, 2, 3), (1, 3, 2, 0), (2, 1, 3, 3))


def kernel(
    sizes, width, lead, den, fj, fi, fk, out, field, flow, k_send, k_recv, k_relay,
    load_sem, south_send, south_recv, east_send, east_recv, down_send, down_recv, relay_send, relay_recv, pair_sem,
):
    _, n_east, n_down = sizes
    nj, ni, nk, ns = den.shape
    chunks = ni // width
    half = n_down // 2
    assert chunks == len(ROUTES[0]) == half
    south, east, down = (lax.axis_index(a) for a in ("south", "east", "down"))
    has_west, has_east = east > 0, east < n_east - 1
    has_up, has_down = down > 0, down < n_down - 1
    inner_k = pl.ds(PAD, nk)
    my_j = jnp.where(south == 0, nj - 1, 0)
    their_j = jnp.where(south == 0, 0, nj + 1)
    rest_j = jnp.where(south == 0, 0, 1)

    def to(axis, index):
        return dict(device_id={axis: index}, device_id_type=pl.DeviceIdType.MESH)

    def each(cond_low, cond_high, fn):
        for side, cond in ((0, cond_low), (1, cond_high)):
            @pl.when(cond)
            def _(side=side):
                fn(side)

    def row_of(c):
        return width * jnp.where(c == 0, 0, jnp.where(c == 1, chunks - 1, c - 1))

    lower = down < half
    at_seam = jnp.logical_or(down == half - 1, down == half)
    mine = lax.rem(down, half)
    own_end = jnp.where(lower, half - 1, half)
    far_end = jnp.where(lower, half, half - 1)
    far_base = jnp.where(lower, half, 0)
    own_base = jnp.where(lower, 0, half)
    own_side = jnp.where(lower, 0, 1)
    is_relay = jnp.logical_not(at_seam)
    def route(t, c):
        n = ROUTES[t][0]
        for x in range(1, chunks):
            n = jnp.where(c == x, ROUTES[t][x], n)
        return n


    def plane_load(n, first, count):
        return pltpu.make_async_copy(
            den.at[my_j, pl.ds(first, count)], field.at[0, my_j + 1, pl.ds(first + 1, count), inner_k], load_sem.at[n])

    loads = [
        plane_load(0, 0, width),
        plane_load(1, width, ni - width),
        pltpu.make_async_copy(
            den.at[pl.ds(rest_j, nj - 1)], field.at[0, pl.ds(rest_j + 1, nj - 1), pl.ds(1, ni), inner_k], load_sem.at[2]),
    ]
    for x, src in enumerate((fj, fi, fk)):
        loads.append(pltpu.make_async_copy(src, flow.at[x], load_sem.at[x + 3]))

    even = lax.rem(east, 2) == 0
    odd = jnp.logical_not(even)
    base = east - lax.rem(east, 2)
    hub = base + 1
    barrier = pltpu.get_barrier_semaphore()

    def hello(cond, index, **others):
        @pl.when(cond)
        def _():
            pl.semaphore_signal(
                barrier, inc=1, device_id={"east": index, **others}, device_id_type=pl.DeviceIdType.MESH)

    near_up = jnp.logical_and(has_up, down != half)
    near_down = jnp.logical_and(has_down, down != half - 1)
    loads[0].start()
    hello(down >= 0, hub, south=1 - south)
    hello(even, hub)
    hello(jnp.logical_and(even, has_west), east - 2, south=0)
    hello(jnp.logical_and(odd, has_east), east + 1, south=0)
    hello(near_up, base, south=0, down=down - 1)
    hello(near_down, base, south=0, down=down + 1)
    hello(is_relay, base, south=0, down=own_end)
    for m in range(half):
        hello(at_seam, base, south=1, down=far_base + m)

    def one(cond, n):
        return jnp.where(cond, n, 0)

    def learn(n, who, count):
        taker = jnp.logical_and(even, south == who)

        @pl.when(taker)
        def _():
            pl.semaphore_wait(barrier, count)
            for s, e in ((who, hub), (1 - who, hub), (1 - who, base)):
                pl.semaphore_signal(
                    pair_sem.at[n], inc=1, device_id={"south": s, "east": e}, device_id_type=pl.DeviceIdType.MESH)

        @pl.when(jnp.logical_not(taker))
        def _():
            pl.semaphore_wait(pair_sem.at[n], 1)

    for copy in loads[1:3]:
        copy.start()

    def south_copy(t, c, part=None):
        if part is None:
            rows = pl.ds(row_of(c) + 1, width)
        else:
            rows = pl.ds(row_of(c) + 1 + part * (width // PARTS), width // PARTS)
            c = chunks - 1 + part
        return pltpu.make_async_remote_copy(
            src_ref=field.at[t, my_j + 1, rows, inner_k], dst_ref=field.at[t, their_j, rows, inner_k],
            send_sem=south_send.at[t, c], recv_sem=south_recv.at[t, c], **to("south", 1 - south))

    def east_copy(t, side):
        r, dst, other = (1, ni + 1, east - 1) if side == 0 else (ni, 0, east + 1)
        return pltpu.make_async_remote_copy(
            src_ref=field.at[t, pl.ds(1, nj), r, inner_k], dst_ref=field.at[t, pl.ds(1, nj), dst, inner_k],
            send_sem=east_send.at[t, side], recv_sem=east_recv.at[t, 1 - side], **to("east", other))

    def down_copy(t, c, side):
        other = down - 1 if side == 0 else down + 1
        return pltpu.make_async_remote_copy(
            src_ref=k_send.at[t, side, c], dst_ref=k_recv.at[t, 1 - side, c],
            send_sem=down_send.at[t, c, side], recv_sem=down_recv.at[t, c, 1 - side], **to("down", other))

    def detour_copy(t, c, side):
        return pltpu.make_async_remote_copy(
            src_ref=k_send.at[t, side, c], dst_ref=k_relay.at[t, c],
            send_sem=down_send.at[t, c, side], recv_sem=relay_recv.at[t, c],
            **to("down", own_base + route(t, c)))

    def hand_on_copy(t, c, side):
        return pltpu.make_async_remote_copy(
            src_ref=k_relay.at[t, c], dst_ref=k_recv.at[t, side, c],
            send_sem=relay_send.at[t, c], recv_sem=down_recv.at[t, c, side], **to("down", far_end))

    def send_down(t, c, near=None):
        def one(side):
            crosses = down == (half if side == 0 else half - 1)
            around = jnp.logical_and(crosses, own_base + route(t, c) != own_end)
            far = jnp.logical_and(crosses, jnp.logical_not(around))
            straight = jnp.logical_not(around)
            if near is not None:
                straight = far if not near else jnp.logical_not(crosses)

            if near is not False:
                @pl.when(around)
                def _():
                    detour_copy(t, c, side).start()

            @pl.when(straight)
            def _():
                down_copy(t, c, side).start()

        each(has_up, has_down, one)

    def hand_on(t, n):
        @pl.when(jnp.logical_and(is_relay, route(t, n) == mine))
        def _():
            pltpu.make_async_remote_copy(
                src_ref=k_relay.at[t, n], dst_ref=k_relay.at[t, n],
                send_sem=relay_send.at[t, n], recv_sem=relay_recv.at[t, n], **to("down", far_end)).wait_recv()
            hand_on_copy(t, n, own_side).start()

    def ends(t, c, w):
        r = row_of(c) + w + 1
        for j in range(nj):
            yield j + 1, r, pl.ds(w * nj + j, 1)

    def pack(t, c):
        def row(w, _):
            for j, r, at in ends(t, c, w):
                k_send[t, 0, c, at] = field[t, j, r, pl.ds(PAD, 1)]
                k_send[t, 1, c, at] = field[t, j, r, pl.ds(PAD + nk - 1, 1)]
            return 0

        lax.fori_loop(0, width, row, 0)

    def unpack(t, c):
        def row(w, _):
            for j, r, at in ends(t, c, w):
                field[t, j, r, pl.ds(PAD - 1, 1)] = k_recv[t, 0, c, at]
                field[t, j, r, pl.ds(PAD + nk, 1)] = k_recv[t, 1, c, at]
            return 0

        lax.fori_loop(0, width, row, 0)

    def advance(t, c, first, count, start=0, rows=width):
        def row(w, _):
            r = row_of(c) + start + w
            for b in range(nk // 8):
                at, here = pl.ds(PAD + 8 * b, 8), pl.ds(8 * b, 8)
                column = [field[t, first + p, r + 1, at] for p in range(count + 2)]
                for p in range(count):
                    j = first + p
                    mid, j_low, j_high = column[p + 1], column[p], column[p + 2]
                    i_low, i_high = field[t, j + 1, r, at], field[t, j + 1, r + 2, at]
                    k_low = field[t, j + 1, r + 1, pl.ds(PAD + 8 * b - 1, 8)]
                    k_high = field[t, j + 1, r + 1, pl.ds(PAD + 8 * b + 1, 8)]
                    spread = j_low + j_high + i_low + i_high + k_low + k_high - 6.0 * mid
                    value = (
                        mid - flow[0, j, r, here] * (j_high - j_low) - flow[1, j, r, here] * (i_high - i_low)
                        - flow[2, j, r, here] * (k_high - k_low) + SMOOTH * spread
                    )
                    if t == STEPS - 1:
                        out[j, r, here] = value
                    else:
                        field[t + 1, j + 1, r + 1, at] = value
            return 0

        lax.fori_loop(0, rows, row, 0, unroll=2)

    loads[0].wait()

    @pl.when(odd)
    def _():
        pl.semaphore_wait(barrier, 3)
        pl.semaphore_signal(pair_sem.at[0], inc=1, **to("east", east - 1))

    @pl.when(even)
    def _():
        pl.semaphore_wait(pair_sem.at[0], 1)

    south_copy(0, 0).start()
    for copy in loads[3:]:
        copy.start()
    loads[1].wait()
    loads[2].wait()

    def first_pack(c, _):
        pack(0, c)
        return 0

    lax.fori_loop(0, chunks, first_pack, 0)
    learn(1, 0, one(base > 0, 2) + one(base + 2 < n_east, 2) + one(near_up, 4) + one(near_down, 4)
          + one(at_seam, 4 * (half - 1)))
    each(has_west, has_east, lambda side: east_copy(0, side).start())

    def first_down(c, _):
        send_down(0, c, True)
        return 0

    lax.fori_loop(0, chunks, first_down, 0)

    outside_j = jnp.where(south == 0, 0, nj + 1)

    def clear(n, _):
        for t in range(STEPS):
            field[t, outside_j, n + 1, inner_k] = jnp.zeros((nk, ns), jnp.float32)
        return 0

    lax.fori_loop(0, ni, clear, 0)
    for edge, at in ((jnp.logical_not(has_west), 0), (jnp.logical_not(has_east), ni + 1)):
        @pl.when(edge)
        def _(at=at):
            for t in range(STEPS):
                for j in range(nj):
                    field[t, j + 1, at, inner_k] = jnp.zeros((nk, ns), jnp.float32)
    for edge, side in ((jnp.logical_not(has_up), 0), (jnp.logical_not(has_down), 1)):
        @pl.when(edge)
        def _(side=side):
            for t in range(STEPS):
                for c in range(chunks):
                    k_recv[t, side, c] = jnp.zeros(k_recv.shape[3:], jnp.float32)

    learn(2, 1, 4)

    def first_far(c, _):
        send_down(0, c, False)
        return 0

    lax.fori_loop(0, chunks, first_far, 0)
    for n in range(chunks):
        hand_on(0, jnp.int32(n))
    for c in range(1, lead):
        south_copy(0, c).start()
    for copy in loads[3:]:
        copy.wait()

    def pass_on(t, c):
        if t < STEPS - 1:
            @pl.when(c > 0)
            def _():
                hand_on(t + 1, c - 1)

        if t > 0:
            @pl.when(c == 0)
            def _():
                hand_on(t, c + chunks - 1)

    def arrive(t, c):
        south_copy(t, c).wait_recv()
        pass_on(t, c)

        @pl.when(c + lead < chunks - (1 if t == STEPS - 1 else 0))
        def _():
            south_copy(t, c + lead).start()

        if t == STEPS - 1:
            @pl.when(c + lead == chunks - 1)
            def _():
                for part in range(PARTS):
                    south_copy(t, chunks - 1, part).start()

        if t < STEPS - 1:
            @pl.when(c + lead >= chunks)
            def _():
                south_copy(t + 1, c + lead - chunks).start()

    def surround(t, c):
        each(has_up, has_down, lambda side: down_copy(t, c, 1 - side).wait_recv())
        for side, cond in ((0, has_west), (1, has_east)):
            @pl.when(jnp.logical_and(cond, c == side))
            def _(side=side):
                east_copy(t, 1 - side).wait_recv()

        unpack(t, c)

    def sent(t, c):
        south_copy(t, c).wait_send()
        each(has_up, has_down, lambda side: down_copy(t, c, side).wait_send())

    for t in range(STEPS - 1):
        def chunk(c, _, t=t):
            arrive(t, c)
            surround(t, c)
            advance(t, c, 0, nj)
            pack(t + 1, c)
            send_down(t + 1, c)
            for side, cond in ((0, has_west), (1, has_east)):
                @pl.when(jnp.logical_and(cond, c == side))
                def _(side=side):
                    east_copy(t + 1, side).start()
            return 0

        lax.fori_loop(0, chunks, chunk, 0)

    t = STEPS - 1

    def last_chunk(c, _):
        early = c + lead < chunks

        @pl.when(early)
        def _():
            arrive(t, c)

        surround(t, c)
        advance(t, c, rest_j, nj - 1)

        @pl.when(c == chunks - 1)
        def _():
            def finish(n, _):
                for s in range(STEPS - 1):
                    sent(s, n)
                each(has_up, has_down, lambda side: down_copy(t, n, side).wait_send())
                return 0

            lax.fori_loop(0, chunks, finish, 0)
            for s in range(STEPS):
                each(has_west, has_east, lambda side: east_copy(s, side).wait_send())
                for n in range(chunks):
                    @pl.when(jnp.logical_and(is_relay, ROUTES[s][n] == mine))
                    def _(s=s, n=n):
                        hand_on_copy(s, n, 0).wait_send()

        @pl.when(jnp.logical_not(jnp.logical_or(early, c == chunks - 1)))
        def _():
            south_copy(t, c).wait_recv()

        @pl.when(c < chunks - 1)
        def _():
            advance(t, c, my_j, 1)

        @pl.when(c == chunks - 1)
        def _():
            for part in range(PARTS):
                south_copy(t, chunks - 1, part).wait_recv()
                advance(t, c, my_j, 1, part * (width // PARTS), width // PARTS)

        return 0

    lax.fori_loop(0, chunks, last_chunk, 0)
    for c in range(chunks - 1):
        south_copy(t, c).wait_send()
    for part in range(PARTS):
        south_copy(t, chunks - 1, part).wait_send()


def store_kernel(pieces, held, out, sem):
    nj, ni = held.shape[:2]
    step = nj * ni // pieces
    copies = [
        pltpu.make_async_copy(
            held.at[p * step // ni, pl.ds(p * step % ni, step)], out.at[p * step // ni, pl.ds(p * step % ni, step)], sem.at[p])
        for p in range(pieces)
    ]
    for copy in copies:
        copy.start()
    for copy in copies:
        copy.wait()


def solution(mesh, width=8, lead=2):
    sizes = tuple(mesh.shape[a] for a in ("south", "east", "down"))

    def per_device(density, flow_j, flow_i, flow_k):
        nj, ni, nk, ns = density.shape
        chunks = ni // width
        dma = pltpu.SemaphoreType.DMA
        held = pl.pallas_call(
            functools.partial(kernel, sizes, width, lead),
            out_shape=pltpu.VMEM(density.shape, density.dtype),
            in_specs=[pl.BlockSpec(memory_space=pl.ANY)] * 4,
            out_specs=pl.BlockSpec(memory_space=pltpu.VMEM),
            scratch_shapes=[
                pltpu.VMEM((STEPS, nj + 2, ni + 2, nk + 2 * PAD, ns), jnp.float32),
                pltpu.VMEM((3, nj, ni, nk, ns), jnp.float32),
                pltpu.VMEM((STEPS, 2, chunks, width * nj, ns), jnp.float32),
                pltpu.VMEM((STEPS, 2, chunks, width * nj, ns), jnp.float32),
                pltpu.VMEM((STEPS, chunks, width * nj, ns), jnp.float32),
                dma((6,)),
                dma((STEPS, chunks + PARTS - 1)),
                dma((STEPS, chunks + PARTS - 1)),
                dma((STEPS, 2)),
                dma((STEPS, 2)),
                dma((STEPS, chunks, 2)),
                dma((STEPS, chunks, 2)),
                dma((STEPS, chunks)),
                dma((STEPS, chunks)),
                pltpu.SemaphoreType.REGULAR((3,)),
            ],
            compiler_params=pltpu.CompilerParams(
                collective_id=0, has_side_effects=True, vmem_limit_bytes=48 * 1024 * 1024
            ),
            name="advect",
        )(density, flow_j, flow_i, flow_k)
        return pl.pallas_call(
            functools.partial(store_kernel, nj),
            out_shape=jax.ShapeDtypeStruct(density.shape, density.dtype),
            in_specs=[pl.BlockSpec(memory_space=pltpu.VMEM)],
            out_specs=pl.BlockSpec(memory_space=pl.ANY),
            scratch_shapes=[dma((nj,))],
            compiler_params=pltpu.CompilerParams(vmem_limit_bytes=8 * 1024 * 1024),
            name="store",
        )(held)

    spec = P(("ens", "south"), "east", "down", None)
    return jax.shard_map(per_device, mesh=mesh, in_specs=(spec,) * 4, out_specs=spec, check_vma=False)
```
